32 devices in a mesh: pb: 2 (over x), col: 16 (over z, y, core).
Axes of the slice: x: 2, y: 2, z: 4, core: 2. Of those that a mesh axis runs over, the one named last changes fastest.
Arguments:
- queries: bfloat16 [4096, 1024], P(('pb', 'col')), may hold values from -64 to 64
- candidates: bfloat16 [16384, 1024], P(('col', 'pb')), may hold values from -5 to 5
- grades: int32 [4096, 16384], P('pb', 'col'), may hold values from 0 to 4
- query_weights: float32 [4096], P('pb'), may hold values from -0.046875 to 0.046875
Outputs:
- losses: float32 [4096], P('pb')
- query_grad: bfloat16 [4096, 1024], P(('pb', 'col'))
- cand_grad: bfloat16 [16384, 1024], P(('col', 'pb'))
The draws below stay inside these ranges and needn't reach their ends.
All inputs are finite; a program needn't handle non-finite values.
Results may differ from the reference program's by a relative error of at most 0.0071.
Values may be sent and summed in bfloat16 or wider, within the bound.
A program may use at most 128 MiB of HBM per device.

```python
import math
import jax
import jax.numpy as jnp
from jax import lax

D = 1024
GRADES = 5
NQ = 4096
NC = 16384


def embed_pair(key):
    query_key = jax.random.fold_in(key, 11)
    cand_key = jax.random.fold_in(key, 12)
    candidates = jnp.clip(jax.random.normal(cand_key, (NC, D), jnp.float32), -5.0, 5.0)
    queries = jnp.clip(jax.random.normal(query_key, (NQ, D), jnp.float32), -5.0, 5.0)
    return (queries, candidates)


def draw_queries(key, part):
    queries, candidates = embed_pair(key)
    return queries.astype(jnp.bfloat16)


def draw_candidates(key, part):
    queries, candidates = embed_pair(key)
    return candidates.astype(jnp.bfloat16)


def draw_grades(key, part):
    kind_key = jax.random.fold_in(key, 21)
    single_key = jax.random.fold_in(key, 22)
    cell_key = jax.random.fold_in(key, 23)
    kinds = jax.random.randint(kind_key, (NQ, 1), 0, 16)
    single = jax.random.randint(single_key, (NQ, 1), 0, GRADES)
    cells = jax.random.randint(cell_key, (NQ, NC), 0, 60)
    spread = cells % GRADES
    upper = 1 + cells % 4
    middle = 2 + cells % 2
    lower = cells % 3
    grades = jnp.where(kinds == 0, upper, jnp.where(kinds == 1, middle, jnp.where(kinds == 2, single, jnp.where(kinds == 3, lower, spread))))
    return grades.astype(jnp.int32)


def steps_of(key, dims, split, smallest, high):
    factor_of, own = 1.0, jax.random.fold_in(key, 6)
    for position, shards_of in split:
        heights = jnp.exp(jax.random.uniform(jax.random.fold_in(own, position), (shards_of,), jnp.float32, smallest / len(split), high / len(split)))
        factor_of = factor_of * jnp.repeat(heights, dims[position] // shards_of).reshape([-1 if axis == position else 1 for axis in range(len(dims))])
    return factor_of


def noise(rng, dims, scale, limit, split=(), held_as=jnp.bfloat16):
    result = scale * jax.random.normal(rng, dims, jnp.float32)
    if split:
        result = result * steps_of(rng, dims, split, -0.22, 0.18)
    return jnp.clip(result, -limit, limit).astype(held_as)


def setup_inputs(seed: int = 0) -> dict:
    streams_of = jax.random.split(jax.random.key(seed), 5)
    return {
        "queries": draw_queries(jax.random.fold_in(streams_of[4], 71), 0),
        "candidates": draw_candidates(jax.random.fold_in(streams_of[4], 71), 0),
        "grades": draw_grades(jax.random.fold_in(streams_of[4], 71), 0),
        "query_weights": noise(streams_of[3], (NQ,), NC ** -0.5, 0.046875, ((0, 2),), jnp.float32),
    }


lowest = -1e+30

def grade_levels(maxima, masses, counts):
    levels = []
    running = maxima[0]
    seen_count = counts[0] * 0.0
    for bucket in range(len(maxima)):
        running = jnp.maximum(running, maxima[bucket])
        seen_count = seen_count + counts[bucket]
        summed = masses[0] * jnp.exp(maxima[0] - running)
        for lesser in range(1, bucket + 1):
            summed = summed + masses[lesser] * jnp.exp(maxima[lesser] - running)
        present = seen_count > 0.0
        levels.append(jnp.where(present, running + jnp.log(jnp.where(present, summed, 1.0)), running))
    return levels

def slope_factors(maxima, levels, counts):
    factors = []
    for bucket in range(len(maxima)):
        summed = counts[bucket] * jnp.exp(maxima[bucket] - levels[bucket])
        for higher in range(bucket + 1, len(maxima)):
            summed = summed + counts[higher] * jnp.exp(maxima[bucket] - levels[higher])
        factors.append(summed)
    return factors

def block_terms(scores, grade_block, weights):
    maxima, masses, counts = ([], [], [])
    for bucket in range(GRADES):
        member = grade_block == bucket
        highest = lax.optimization_barrier(jnp.max(jnp.where(member, scores, lowest), axis=1))
        masses.append(lax.optimization_barrier(jnp.sum(jnp.exp(jnp.where(member, scores - highest[:, None], lowest)), axis=1)))
        counts.append(lax.optimization_barrier(jnp.sum(member.astype(jnp.float32), axis=1)))
        maxima.append(highest)
    totals = lax.optimization_barrier(jnp.sum(scores, axis=1))
    levels = grade_levels(maxima, masses, counts)
    weighted = counts[0] * levels[0]
    for bucket in range(1, GRADES):
        weighted = weighted + counts[bucket] * levels[bucket]
    losses = (weighted - totals) / NC
    factors = slope_factors(maxima, levels, counts)
    picked_factor = jnp.zeros(scores.shape, jnp.float32)
    picked_max = jnp.zeros(scores.shape, jnp.float32)
    for bucket in range(GRADES):
        member = grade_block == bucket
        picked_factor = jnp.where(member, factors[bucket][:, None], picked_factor)
        picked_max = jnp.where(member, maxima[bucket][:, None], picked_max)
    slopes = (weights[:, None] * (picked_factor * jnp.exp(scores - picked_max) - 1.0)).astype(jnp.bfloat16)
    return (losses, slopes)

def reference(queries, candidates, grades, query_weights):
    scaling = 1.0 / math.sqrt(D)
    block_rows = math.gcd(NQ, 256)
    blocks = NQ // block_rows
    query_blocks = queries.reshape(blocks, block_rows, D)
    grade_blocks = grades.reshape(blocks, block_rows, NC)
    weight_blocks = query_weights.reshape(blocks, block_rows)

    def advance(cand_total, pieces):
        row_block, grade_block, weights = pieces
        scores = jnp.dot(row_block, candidates.T, preferred_element_type=jnp.float32) * scaling
        losses, slopes = block_terms(scores, grade_block, weights)
        query_part = (jnp.dot(slopes, candidates, preferred_element_type=jnp.float32) * scaling).astype(jnp.bfloat16)
        cand_total = cand_total + lax.dot_general(slopes, row_block, (((0,), (0,)), ((), ())), preferred_element_type=jnp.float32)
        return (cand_total, (losses, query_part))
    initial = jnp.zeros((NC, D), jnp.float32)
    final, (losses, query_parts) = lax.scan(advance, initial, (query_blocks, grade_blocks, weight_blocks))
    return (losses.reshape(NQ), query_parts.reshape(NQ, D), (final * scaling).astype(jnp.bfloat16))
```

```python
import functools
import math

import jax
import jax.numpy as jnp
from jax import lax
from jax.experimental import pallas as pl
from jax.experimental.pallas import tpu as pltpu
from jax.sharding import PartitionSpec as P

GRADES = 5
STATS = 16
LOWEST = -1e30
LANES = 128
SUBS = 2
MESH = pl.DeviceIdType.MESH
F32 = jnp.float32
BF16 = jnp.bfloat16
LOG2E = math.log2(math.e)
LN2 = math.log(2.0)


class Place:
    def __init__(self, n_col, n_pb):
        assert n_col % 4 == 0
        self.n_col, self.n_pb = n_col, n_pb
        self.cores = self.mids = 2
        self.chips = n_col // 2
        self.outs = n_col // 4
        self.me = lax.axis_index("col")
        self.p = lax.axis_index("pb")
        self.core = lax.rem(self.me, 2)
        self.mid = lax.rem(self.me // 2, 2)
        self.out = self.me // 4

    def chip(self, out, dm):
        return out * 2 + lax.rem(self.mid + dm, 2)

    def block(self, out, dm, dc):
        return self.chip(out, dm) * 2 + lax.rem(self.core + dc, 2)

    def dev(self, col):
        return {"pb": self.p, "col": col}

    def visit(self, k):
        side = jnp.minimum(self.out, self.outs - 1 - self.out)
        near = (k + 1) // 2 * (2 * lax.rem(k, 2) - 1)
        far = (k - side) * jnp.where(2 * self.out < self.outs, 1, -1)
        return self.out + jnp.where(k <= 2 * side, near, far)

    def item(self, t):
        odd = (lax.rem(t, 2) == 1) & (t < self.chips - 1)
        first = t == 0
        v = jnp.where(odd, self.outs - 1 - (t + 1) // 2, self.outs - 1 - (t - 1) // 2)
        v = jnp.where(first, self.outs - 1, v)
        dm = jnp.where(odd | first, 1, 0)
        return self.visit(v), dm


def remote(src, dst, send, recv, device):
    return pltpu.make_async_remote_copy(
        src_ref=src, dst_ref=dst, send_sem=send, recv_sem=recv, device_id=device, device_id_type=MESH
    )


def span(block, size):
    return pl.ds(pl.multiple_of(block * size, size), size)


def stats_table(s, g):
    rows = s.shape[0]
    lane = lax.broadcasted_iota(jnp.int32, (rows, LANES), 1)
    tops = [jnp.max(jnp.where(g <= b, s, LOWEST), axis=1, keepdims=True) for b in range(GRADES - 1)]
    tops.append(jnp.max(s, axis=1, keepdims=True))
    picked = tops[-1]
    for b in range(GRADES - 2, -1, -1):
        picked = jnp.where(g <= b, tops[b], picked)
    e = jnp.exp2(s - picked)
    sums = [jnp.sum(jnp.where(g <= b, e, 0.0), axis=1, keepdims=True) for b in range(GRADES - 1)]
    sums.append(jnp.sum(e, axis=1, keepdims=True))
    table = jnp.where(lane == 2 * GRADES, jnp.sum(s, axis=1, keepdims=True), 0.0)
    for b in range(GRADES):
        table = jnp.where(lane == b, tops[b], table)
        table = jnp.where(lane == GRADES + b, sums[b], table)
    return table


def count_table(g):
    rows, cols = g.shape
    assert cols % LANES == 0 and cols // LANES < 16 and cols < 4096
    code = jnp.zeros((rows, LANES), jnp.int32)
    for k in range(0, cols, LANES):
        code = code + jnp.left_shift(1, g[:, k : k + LANES] * 4)
    lane = lax.broadcasted_iota(jnp.int32, (rows, LANES), 1)
    table = jnp.zeros((rows, LANES), F32)
    for b in range(0, GRADES - 1, 2):
        low = jnp.right_shift(code, 4 * b) & 15
        high = jnp.right_shift(code, 4 * b + 4) & 15
        pair = jnp.sum((low + high * 4096).astype(F32), axis=1, keepdims=True)
        high = jnp.floor(pair * (1.0 / 4096.0))
        table = jnp.where(lane == b, pair - high * 4096.0, table)
        table = jnp.where(lane == b + 1, high, table)
    return table


def finish(got, n_col, cols, columns):
    G = GRADES
    tops = got[0][:G]
    for k in range(1, n_col):
        tops = jnp.maximum(tops, got[k][:G])
    masses = jnp.zeros_like(tops)
    rest = jnp.zeros((STATS - 2 * G, tops.shape[1]), F32)
    for k in range(n_col):
        block = got[k]
        masses = masses + block[G : 2 * G] * jnp.exp2(block[:G] - tops)
        rest = rest + block[2 * G :]
    top = [tops[b : b + 1] for b in range(G)]
    mass = [masses[b : b + 1] for b in range(G)]
    total = rest[:1]
    count = [rest[b + 1 : b + 2] for b in range(G - 1)]
    count.append(float(cols * n_col) - (count[0] + count[1] + count[2] + count[3]))
    levels = []
    seen = jnp.zeros_like(total)
    summed = seen
    weighted = seen
    for b in range(G):
        seen = seen + count[b]
        summed = mass[b] if b == 0 else mass[b] + summed * jnp.exp2(top[b - 1] - top[b])
        present = seen > 0.0
        level = jnp.where(present, top[b] + jnp.log(jnp.where(present, summed, 1.0)) * LOG2E, top[b])
        levels.append(level)
        weighted = weighted + count[b] * level
    loss = (weighted - total) * (LN2 / columns)
    offsets = [None] * G
    factor = seen * 0.0
    for b in range(G - 1, -1, -1):
        own = count[b] * jnp.exp2(top[b] - levels[b])
        factor = own if b == G - 1 else own + factor * jnp.exp2(top[b] - top[b + 1])
        offsets[b] = jnp.log(jnp.maximum(factor, 1e-37)) * LOG2E - top[b]
    pad = jnp.zeros((8 - G - 1, loss.shape[1]), F32)
    return jnp.concatenate(offsets + [loss, pad], axis=0)


def kernel(
    n_col, n_pb, pieces, scaling, columns,
    q_hbm, c_hbm, g_hbm, w_ref, loss_ref, q_out, c_out,
    q_all, c_all, g_all, s_all, slopes, tables, counts, stats, got, mine, merged,
    q_part, core_got, y_got, z_got, z_part, acc, c_part, c_own, c_got,
    own_sem, g_sem, q_send, q_recv, c_send, c_recv, s_send, s_recv, m_send, m_recv,
    k_send, k_recv, y_send, y_recv, z_send, z_recv, x_send, x_recv,
):
    at = Place(n_col, n_pb)
    rows, width = q_hbm.shape
    half = c_hbm.shape[0]
    cols = half * n_pb
    pair = 2 * rows
    sub = rows // SUBS
    outs, chips = at.outs, at.chips
    G = GRADES
    wide = half // pieces
    far_parts = [(d, s) for s in range(pieces) for d in range(1, n_pb)]
    n_far = len(far_parts)

    own_q = pltpu.make_async_copy(q_hbm, q_all.at[span(at.me, rows)], own_sem.at[0])
    own_c = pltpu.make_async_copy(c_hbm, c_all.at[span(at.p, half)], own_sem.at[1])
    own_q.start()
    own_c.start()

    def grades_in(k, start):
        for dm in range(2):
            chip = at.chip(at.visit(k), dm)
            copy = pltpu.make_async_copy(g_hbm.at[span(chip, pair)], g_all.at[span(chip, pair)], g_sem.at[chip])
            copy.start() if start else copy.wait()

    for k in range(outs):
        grades_in(k, True)
    barrier = pltpu.get_barrier_semaphore()
    for d in range(1, n_col):
        pl.semaphore_signal(
            barrier, inc=1, device_id=at.dev(lax.rem(at.me + d, n_col)), device_id_type=MESH
        )
    for d in range(1, n_pb):
        pl.semaphore_signal(
            barrier, inc=1, device_id={"pb": lax.rem(at.p + d, n_pb), "col": at.me}, device_id_type=MESH
        )
    pl.semaphore_wait(barrier, n_col + n_pb - 2)

    def q_span(block, s):
        return pl.ds(pl.multiple_of(block * rows + s * sub, sub), sub)

    def q_copy(block, s, t, col):
        ref = q_all.at[q_span(block, s)]
        return remote(ref, ref, q_send.at[block, t, s], q_recv.at[block, s], at.dev(col))

    def forward(k, dm, act):
        out = at.visit(k)
        block = at.block(out, dm, 0)
        for s in range(SUBS):
            if act and not (isinstance(k, int) and k == 0 and dm == 0):
                q_copy(block, s, 0, at.me).wait_recv()

            def go(t, col):
                copy = q_copy(block, s, t, col)
                copy.start() if act else copy.wait_send()

            if dm == 0:
                @pl.when((out <= at.out) & (at.out < outs - 1))
                def _():
                    go(0, at.block(at.out + 1, 0, 0))

                @pl.when((out >= at.out) & (at.out > 0))
                def _():
                    go(1, at.block(at.out - 1, 0, 0))

                go(2, at.block(at.out, 1, 0))
            go(3, at.block(at.out, 0, 1))

    def partner(k, dm):
        block = at.block(at.visit(k), dm, 1)
        for s in range(SUBS):
            q_copy(block, s, 0, at.me).wait_recv()

    def c_copy(d, s):
        ref = c_all.at[pl.ds(pl.multiple_of(at.p * half + s * wide, wide), wide)]
        other = lax.rem(at.p + d, n_pb)
        return remote(ref, ref, c_send.at[d, s], c_recv.at[at.p, s], {"pb": other, "col": at.me})

    def c_arrived(d, s):
        other = lax.rem(at.p + d, n_pb)
        ref = c_all.at[pl.ds(pl.multiple_of(other * half + s * wide, wide), wide)]
        remote(ref, ref, c_send.at[d, s], c_recv.at[other, s], at.dev(at.me)).wait_recv()

    own_q.wait()
    forward(0, 0, True)
    own_c.wait()
    for d, s in far_parts:
        c_copy(d, s).start()

    def score(k, dm, start, size, part):
        chip = at.chip(at.visit(k), dm)
        columns_ = pl.ds(pl.multiple_of(start, size), size)
        rr = span(chip, pair)
        s = lax.dot_general(
            q_all[rr], c_all[columns_], (((1,), (1,)), ((), ())), preferred_element_type=F32
        ) * (scaling * LOG2E)
        s_all[rr, columns_] = s
        for c in range(2):
            block = chip * 2 + c
            g = g_all[span(block, rows), columns_]
            tables[block, part] = stats_table(s[c * rows : (c + 1) * rows], g).T[:STATS]

    def near(k, dm):
        score(k, dm, at.p * half, half, 0)

    def far(k, dm, r):
        d, s = far_parts[r] if isinstance(r, int) else (1 + lax.rem(r, n_pb - 1), r // (n_pb - 1))
        start = lax.rem(at.p + d, n_pb) * half + s * wide
        score(k, dm, start, wide, r + 1)

    def count(block, carry):
        counts[block] = count_table(g_all[span(block, rows), :]).T[:8]
        return carry

    partner(0, 0)
    for k in range(outs):
        grades_in(k, False)
    early = n_far // 2

    def step(u, carry):
        @pl.when((u > 0) & (u < outs))
        def _():
            forward(u, 0, True)

        @pl.when((u > 0) & (u <= outs))
        def _():
            forward(u - 1, 1, True)
            partner(u - 1, 1)
            near(u - 1, 1)

        @pl.when((u > 0) & (u < outs))
        def _():
            partner(u, 0)

        @pl.when(u < outs)
        def _():
            near(u, 0)

        @pl.when(u == 0)
        def _():
            lax.fori_loop(0, n_col, count, 0)

        @pl.when(u >= 2)
        def _():
            @pl.when(u == 2)
            def _():
                for r in range(early):
                    c_arrived(*far_parts[r])

            def body(j, c):
                far(u - 2, lax.rem(j, 2), j // 2)
                return c

            lax.fori_loop(0, 2 * early, body, 0)

        return carry

    lax.fori_loop(0, outs + 2, step, 0)
    for r in range(early, n_far):
        c_arrived(*far_parts[r])

    def stat_copy(block):
        return remote(stats.at[block], got.at[at.me], s_send.at[block], s_recv.at[at.me], at.dev(block))

    def last(j, carry):
        k, dm = outs - 1 - j // 2, 1 - lax.rem(j, 2)

        def body(r, c):
            far(k, dm, r)
            return c

        lax.fori_loop(early, n_far, body, 0)
        for c in range(2):
            block = at.chip(at.visit(k), dm) * 2 + c
            parts = [tables[block, h] for h in range(n_far + 1)]
            top = parts[0][:G]
            for part in parts[1:]:
                top = jnp.maximum(top, part[:G])
            mass = jnp.zeros_like(top)
            total = jnp.zeros((1, rows), F32)
            for part in parts:
                upto = part[G : 2 * G]
                own = jnp.concatenate([upto[:1], upto[1:] - upto[:-1]], axis=0)
                mass = mass + own * jnp.exp2(part[:G] - top)
                total = total + part[2 * G : 2 * G + 1]
            pad = jnp.zeros((1, rows), F32)
            stats[block] = jnp.concatenate([top, mass, total, counts[block, :4], pad], axis=0)

            @pl.when(block != at.me)
            def _():
                stat_copy(block).start()

        return carry

    lax.fori_loop(0, chips, last, 0)

    others = [lax.rem(at.me + d, n_col) for d in range(1, n_col)]
    got[at.me] = stats[at.me]
    for o in others:
        remote(stats.at[o], got.at[o], s_send.at[o], s_recv.at[o], at.dev(at.me)).wait_recv()
    mine[...] = finish(got, n_col, cols, columns)

    def merged_copy(o):
        return remote(mine, merged.at[at.me], m_send.at[o], m_recv.at[at.me], at.dev(o))

    for o in others:
        merged_copy(o).start()
    merged[at.me] = mine[...]
    for o in others:
        remote(mine, merged.at[o], m_send.at[o], m_recv.at[o], at.dev(at.me)).wait_recv()

    step_rows = min(64, rows)

    def slope(block):
        table = jnp.concatenate(
            [merged[block][: G + 1], w_ref[pl.ds(block, 1), :], jnp.zeros((rows - G - 2, rows), F32)], axis=0
        ).T
        loss_ref[pl.ds(block, 1), :] = merged[block][G : G + 1]
        for r in range(0, rows, step_rows):
            rr = pl.ds(pl.multiple_of(block * rows + r, step_rows), step_rows)
            t = table[r : r + step_rows]
            g = g_all[rr, :]
            off = jnp.broadcast_to(t[:, G - 1 : G], g.shape)
            for b in range(G - 2, -1, -1):
                off = jnp.where(g <= b, t[:, b : b + 1], off)
            w = t[:, G + 1 : G + 2]
            slopes[rr, :] = (w * jnp.exp2(s_all[rr, :] + off) - w).astype(BF16)

    def k_copy(chip):
        return remote(
            q_part.at[chip, lax.rem(at.core + 1, 2)], core_got.at[chip], k_send.at[chip], k_recv.at[chip],
            at.dev(at.block(at.out, 0, 1)),
        )

    def q_grad(t):
        out, dm = at.item(t)
        chip = at.chip(out, dm)
        part = jnp.dot(slopes[span(chip, pair), :], c_all[...], preferred_element_type=F32) * scaling
        q_part[chip] = part.astype(BF16).reshape(2, rows, width)
        k_copy(chip).start()

    def sub_rows(s):
        return pl.ds(s * sub, sub)

    def y_copy(out, s):
        return remote(
            q_part.at[at.chip(out, 1), at.core, sub_rows(s)], y_got.at[out, sub_rows(s)],
            y_send.at[out, s], y_recv.at[out, s], at.dev(at.block(at.out, 1, 0)),
        )

    def cross(out):
        chip = at.chip(out, 1)
        k_copy(chip).wait_recv()
        for s in range(SUBS):
            rr = sub_rows(s)
            both = q_part[chip, at.core, rr].astype(F32) + core_got[chip, rr].astype(F32)
            q_part[chip, at.core, rr] = both.astype(BF16)
            y_copy(out, s).start()

    def z_copy(out, s):
        toward = jnp.where(out > at.out, at.out + 1, at.out - 1)
        slot = jnp.where((out < at.out) & (toward == out), outs, out)
        return remote(
            z_part.at[out, sub_rows(s)], z_got.at[slot, sub_rows(s)],
            z_send.at[out, s], z_recv.at[slot, s], at.dev(at.block(toward, 0, 0)),
        )

    def z_add(slot, s):
        ref = z_got.at[slot, sub_rows(s)]
        remote(ref, ref, z_send.at[0, s], z_recv.at[slot, s], at.dev(at.me)).wait_recv()
        acc[...] += z_got[slot, sub_rows(s)].astype(F32)

    def gather_row(out, s):
        chip = at.chip(out, 0)
        rr = sub_rows(s)
        ref = y_got.at[out, rr]
        remote(ref, ref, y_send.at[out, s], y_recv.at[out, s], at.dev(at.me)).wait_recv()
        acc[...] = (
            q_part[chip, at.core, rr].astype(F32)
            + core_got[chip, rr].astype(F32)
            + y_got[out, rr].astype(F32)
        )

    def chain(v):
        out = at.visit(v)
        k_copy(at.chip(out, 0)).wait_recv()
        behind = ((out > at.out) & (at.out > 0)) | ((out < at.out) & (at.out < outs - 1))
        for s in range(SUBS):
            gather_row(out, s)

            @pl.when(behind)
            def _():
                z_add(out, s)

            z_part[out, sub_rows(s)] = acc[...].astype(BF16)
            z_copy(out, s).start()

    chunk = min(LANES, half)
    per = half // chunk
    n_x = per * (n_pb - 1)

    def x_copy(r):
        d, j = 1 + r // per, lax.rem(r, per)
        other = lax.rem(at.p + d, n_pb)
        rr = pl.ds(pl.multiple_of(j * chunk, chunk), chunk)
        return remote(
            c_part.at[r], c_got.at[d - 1, rr], x_send.at[r], x_recv.at[r], {"pb": other, "col": at.me}
        )

    def c_grad(start):
        return lax.dot_general(
            slopes[:, pl.ds(pl.multiple_of(start, chunk), chunk)], q_all[...],
            (((0,), (0,)), ((), ())), preferred_element_type=F32,
        ) * scaling

    def c_far(r):
        other = lax.rem(at.p + 1 + r // per, n_pb)
        c_part[r] = c_grad(other * half + lax.rem(r, per) * chunk).astype(BF16)
        x_copy(r).start()

    def slope_step(i, carry):
        out, dm = at.item(i)
        for c in range(2):
            slope(at.chip(out, dm) * 2 + c)

        @pl.when(i == 0)
        def _():
            q_grad(0)

        @pl.when(i == 2)
        def _():
            cross(at.visit(outs - 1))

        return carry

    lax.fori_loop(0, chips, slope_step, 0)

    def grad_step(j, carry):
        @pl.when(j < n_x)
        def _():
            c_far(j)

        @pl.when(j + 1 < chips)
        def _():
            q_grad(j + 1)

        @pl.when((j >= 1) & (lax.rem(j, 2) == 1) & (j < chips - 1))
        def _():
            cross(at.item(j)[0])

        return carry

    lax.fori_loop(0, max(n_x, chips - 1), grad_step, 0)

    def c_near(j, carry):
        c_own[pl.ds(pl.multiple_of(j * chunk, chunk), chunk)] = c_grad(at.p * half + j * chunk)
        return carry

    def chain_step(i, carry):
        chain(outs - 1 - i)

        @pl.when(i == 0)
        def _():
            lax.fori_loop(0, per, c_near, 0)

        return carry

    lax.fori_loop(0, outs - 1, chain_step, 0)
    k_copy(at.chip(at.out, 0)).wait_recv()
    for s in range(SUBS):
        gather_row(at.out, s)

        @pl.when(at.out > 0)
        def _():
            z_add(at.out, s)

        @pl.when(at.out < outs - 1)
        def _():
            z_add(outs, s)

        q_out[sub_rows(s), :] = acc[...].astype(BF16)

    def c_finish(j, carry):
        rr = pl.ds(pl.multiple_of(j * chunk, chunk), chunk)
        total = c_own[rr]
        for d in range(1, n_pb):
            r = (d - 1) * per + j
            ref = c_got.at[d - 1, rr]
            remote(ref, ref, x_send.at[r], x_recv.at[r], at.dev(at.me)).wait_recv()
            total = total + c_got[d - 1, rr].astype(F32)
        c_out[rr] = total.astype(BF16)
        return carry

    lax.fori_loop(0, per, c_finish, 0)

    def drain(k, carry):
        for dm in range(2):
            forward(k, dm, False)
        out = at.visit(k)
        for dm in range(2):
            k_copy(at.chip(out, dm)).wait_send()
        for s in range(SUBS):
            y_copy(out, s).wait_send()

            @pl.when(k > 0)
            def _():
                z_copy(out, s).wait_send()

        return carry

    lax.fori_loop(0, outs, drain, 0)
    for d, s in far_parts:
        c_copy(d, s).wait_send()
    for o in others:
        stat_copy(o).wait_send()
        merged_copy(o).wait_send()
    lax.fori_loop(0, n_x, lambda r, c: (x_copy(r).wait_send(), c)[1], 0)


def local(queries, candidates, grades, query_weights):
    n_col, n_pb = lax.axis_size("col"), lax.axis_size("pb")
    rows, width = queries.shape
    half = candidates.shape[0]
    tall, cols = grades.shape
    scaling = 1.0 / math.sqrt(width)
    pieces = 2 if half % 256 == 0 else 1
    outs, chips = n_col // 4, n_col // 2
    chunk = min(LANES, half)
    n_x = half // chunk * (n_pb - 1)
    sub = rows // SUBS
    dma = pltpu.SemaphoreType.DMA
    vmem = pl.BlockSpec(memory_space=pltpu.VMEM)
    hbm = pl.BlockSpec(memory_space=pl.ANY)
    losses, query_grad, cand_grad = pl.pallas_call(
        functools.partial(kernel, n_col, n_pb, pieces, scaling, cols * n_col),
        out_shape=(
            jax.ShapeDtypeStruct((n_col, rows), F32),
            jax.ShapeDtypeStruct((rows, width), BF16),
            jax.ShapeDtypeStruct((half, width), BF16),
        ),
        in_specs=[hbm, hbm, hbm, vmem],
        out_specs=(vmem, vmem, vmem),
        scratch_shapes=[
            pltpu.VMEM((tall, width), BF16),
            pltpu.VMEM((cols, width), BF16),
            pltpu.VMEM((tall, cols), jnp.int32),
            pltpu.VMEM((tall, cols), F32),
            pltpu.VMEM((tall, cols), BF16),
            pltpu.VMEM((n_col, 1 + pieces * (n_pb - 1), STATS, rows), F32),
            pltpu.VMEM((n_col, 8, rows), F32),
            pltpu.VMEM((n_col, STATS, rows), F32),
            pltpu.VMEM((n_col, STATS, rows), F32),
            pltpu.VMEM((8, rows), F32),
            pltpu.VMEM((n_col, 8, rows), F32),
            pltpu.VMEM((chips, 2, rows, width), BF16),
            pltpu.VMEM((chips, rows, width), BF16),
            pltpu.VMEM((outs, rows, width), BF16),
            pltpu.VMEM((outs + 1, rows, width), BF16),
            pltpu.VMEM((outs, rows, width), BF16),
            pltpu.VMEM((sub, width), F32),
            pltpu.VMEM((n_x, chunk, width), BF16),
            pltpu.VMEM((half, width), F32),
            pltpu.VMEM((n_pb - 1, half, width), BF16),
            dma((2,)),
            dma((chips,)),
            dma((n_col, 4, SUBS)),
            dma((n_col, SUBS)),
            dma((n_pb, pieces)),
            dma((n_pb, pieces)),
            dma((n_col,)),
            dma((n_col,)),
            dma((n_col,)),
            dma((n_col,)),
            dma((chips,)),
            dma((chips,)),
            dma((outs, SUBS)),
            dma((outs, SUBS)),
            dma((outs, SUBS)),
            dma((outs + 1, SUBS)),
            dma((n_x,)),
            dma((n_x,)),
        ],
        compiler_params=pltpu.CompilerParams(
            collective_id=0, has_side_effects=True, vmem_limit_bytes=62 * 2**20
        ),
        name="listmle",
    )(queries, candidates, grades, query_weights.reshape(n_col, rows))
    return (losses.reshape(-1), query_grad, cand_grad)


def solution(mesh):
    in_specs = (P(("pb", "col"), None), P(("col", "pb"), None), P("pb", "col"), P("pb"))
    out_specs = (P("pb"), P(("pb", "col"), None), P(("col", "pb"), None))
    return jax.shard_map(local, mesh=mesh, in_specs=in_specs, out_specs=out_specs, check_vma=False)
```

```python
import functools
import math

import jax
import jax.numpy as jnp
from jax import lax
from jax.experimental import pallas as pl
from jax.experimental.pallas import tpu as pltpu
from jax.sharding import PartitionSpec as P

GRADES = 5
STATS = 16
LOWEST = -1e30
LANES = 128
SUBS = 2
MESH = pl.DeviceIdType.MESH
F32 = jnp.float32
BF16 = jnp.bfloat16
LOG2E = math.log2(math.e)
LN2 = math.log(2.0)


class Place:
    def __init__(self, n_col, n_pb):
        assert n_col % 4 == 0
        self.n_col, self.n_pb = n_col, n_pb
        self.cores = self.mids = 2
        self.chips = n_col // 2
        self.outs = n_col // 4
        self.me = lax.axis_index("col")
        self.p = lax.axis_index("pb")
        self.core = lax.rem(self.me, 2)
        self.mid = lax.rem(self.me // 2, 2)
        self.out = self.me // 4

    def chip(self, out, dm):
        return out * 2 + lax.rem(self.mid + dm, 2)

    def block(self, out, dm, dc):
        return self.chip(out, dm) * 2 + lax.rem(self.core + dc, 2)

    def dev(self, col):
        return {"pb": self.p, "col": col}

    def visit(self, k):
        side = jnp.minimum(self.out, self.outs - 1 - self.out)
        near = (k + 1) // 2 * (2 * lax.rem(k, 2) - 1)
        far = (k - side) * jnp.where(2 * self.out < self.outs, 1, -1)
        return self.out + jnp.where(k <= 2 * side, near, far)

    def item(self, t):
        odd = (lax.rem(t, 2) == 1) & (t < self.chips - 1)
        first = t == 0
        v = jnp.where(odd, self.outs - 1 - (t + 1) // 2, self.outs - 1 - (t - 1) // 2)
        v = jnp.where(first, self.outs - 1, v)
        dm = jnp.where(odd | first, 1, 0)
        return self.visit(v), dm


def remote(src, dst, send, recv, device):
    return pltpu.make_async_remote_copy(
        src_ref=src, dst_ref=dst, send_sem=send, recv_sem=recv, device_id=device, device_id_type=MESH
    )


def span(block, size):
    return pl.ds(pl.multiple_of(block * size, size), size)


def statistics(s, g, put):
    tops = [jnp.max(jnp.where(g <= b, s, LOWEST), axis=0, keepdims=True) for b in range(GRADES - 1)]
    tops.append(jnp.max(s, axis=0, keepdims=True))
    picked = jnp.broadcast_to(tops[-1], s.shape)
    for b in range(GRADES - 2, -1, -1):
        picked = jnp.where(g <= b, tops[b], picked)
    e = jnp.exp2(s - picked)
    sums = [jnp.sum(jnp.where(g <= b, e, 0.0), axis=0, keepdims=True) for b in range(GRADES - 1)]
    sums.append(jnp.sum(e, axis=0, keepdims=True))
    for i, row in enumerate(tops + sums + [jnp.sum(s, axis=0, keepdims=True)]):
        put(i, row)


def finish(got, n_col, cols, columns):
    G = GRADES
    tops = got[0][:G]
    for k in range(1, n_col):
        tops = jnp.maximum(tops, got[k][:G])
    masses = jnp.zeros_like(tops)
    rest = jnp.zeros((STATS - 2 * G, tops.shape[1]), F32)
    for k in range(n_col):
        block = got[k]
        masses = masses + block[G : 2 * G] * jnp.exp2(block[:G] - tops)
        rest = rest + block[2 * G :]
    top = [tops[b : b + 1] for b in range(G)]
    mass = [masses[b : b + 1] for b in range(G)]
    total = rest[:1]
    count = [rest[b + 1 : b + 2] for b in range(G - 1)]
    count.append(float(cols * n_col) - (count[0] + count[1] + count[2] + count[3]))
    levels = []
    seen = jnp.zeros_like(total)
    summed = seen
    weighted = seen
    for b in range(G):
        seen = seen + count[b]
        summed = mass[b] if b == 0 else mass[b] + summed * jnp.exp2(top[b - 1] - top[b])
        present = seen > 0.0
        level = jnp.where(present, top[b] + jnp.log(jnp.where(present, summed, 1.0)) * LOG2E, top[b])
        levels.append(level)
        weighted = weighted + count[b] * level
    loss = (weighted - total) * (LN2 / columns)
    offsets = [None] * G
    factor = seen * 0.0
    for b in range(G - 1, -1, -1):
        own = count[b] * jnp.exp2(top[b] - levels[b])
        factor = own if b == G - 1 else own + factor * jnp.exp2(top[b] - top[b + 1])
        offsets[b] = jnp.log(jnp.maximum(factor, 1e-37)) * LOG2E - top[b]
    pad = jnp.zeros((8 - G - 1, loss.shape[1]), F32)
    return jnp.concatenate(offsets + [loss, pad], axis=0)


def far_parts_of(half, n_pb):
    sizes = [half // 2, half // 4, half // 4] if half % 512 == 0 else [half]
    return [(d, sum(sizes[:i]), n) for i, n in enumerate(sizes) for d in range(1, n_pb)]


def kernel(
    n_col, n_pb, scaling, columns,
    q_hbm, c_hbm, g_hbm, w_ref, loss_ref, q_out, c_out,
    q_all, c_all, g_raw, g_all, s_all, slopes, tables, counts, stats, got, mine, merged,
    q_part, core_got, y_got, z_got, z_part, acc, c_part, c_own, c_got,
    own_sem, g_sem, q_send, q_recv, c_send, c_recv, s_send, s_recv, m_send, m_recv,
    k_send, k_recv, y_send, y_recv, z_send, z_recv, x_send, x_recv,
):
    at = Place(n_col, n_pb)
    rows, width = q_hbm.shape
    half = c_hbm.shape[0]
    tall, cols = g_hbm.shape
    pair, quad = 2 * rows, 4 * rows
    sub = rows // SUBS
    outs, chips = at.outs, at.chips
    G = GRADES
    parts = far_parts_of(half, n_pb)
    n_far = len(parts)
    early = n_pb - 1

    own_q = pltpu.make_async_copy(q_hbm, q_all.at[span(at.me, rows)], own_sem.at[0])
    own_c = pltpu.make_async_copy(c_hbm, c_all.at[span(at.p, half)], own_sem.at[1])
    own_q.start()
    own_c.start()
    group = 8 * LANES
    g_copies = [
        pltpu.make_async_copy(g_hbm.at[pl.ds(h, group)], g_raw.at[pl.ds(h, group)], g_sem.at[h // group])
        for h in range(0, tall, group)
    ]
    for copy in g_copies:
        copy.start()
    barrier = pltpu.get_barrier_semaphore()
    for d in range(1, n_col):
        pl.semaphore_signal(
            barrier, inc=1, device_id=at.dev(lax.rem(at.me + d, n_col)), device_id_type=MESH
        )
    for d in range(1, n_pb):
        pl.semaphore_signal(
            barrier, inc=1, device_id={"pb": lax.rem(at.p + d, n_pb), "col": at.me}, device_id_type=MESH
        )
    pl.semaphore_wait(barrier, n_col + n_pb - 2)

    def q_span(block, s):
        return pl.ds(pl.multiple_of(block * rows + s * sub, sub), sub)

    def q_copy(block, s, t, col):
        ref = q_all.at[q_span(block, s)]
        return remote(ref, ref, q_send.at[block, t, s], q_recv.at[block, s], at.dev(col))

    def forward(k, dm, act):
        out = at.visit(k)
        block = at.block(out, dm, 0)
        for s in range(SUBS):
            if act and not (isinstance(k, int) and k == 0 and dm == 0):
                q_copy(block, s, 0, at.me).wait_recv()

            def go(t, col):
                copy = q_copy(block, s, t, col)
                copy.start() if act else copy.wait_send()

            if dm == 0:
                @pl.when((out <= at.out) & (at.out < outs - 1))
                def _():
                    go(0, at.block(at.out + 1, 0, 0))

                @pl.when((out >= at.out) & (at.out > 0))
                def _():
                    go(1, at.block(at.out - 1, 0, 0))

                go(2, at.block(at.out, 1, 0))
            go(3, at.block(at.out, 0, 1))

    def partner(k, dm):
        block = at.block(at.visit(k), dm, 1)
        for s in range(SUBS):
            q_copy(block, s, 0, at.me).wait_recv()

    def c_copy(r):
        d, first, n = parts[r]
        ref = c_all.at[pl.ds(pl.multiple_of(at.p * half + first, n), n)]
        other = lax.rem(at.p + d, n_pb)
        return remote(ref, ref, c_send.at[r], c_recv.at[r], {"pb": other, "col": at.me})

    def c_arrived(r):
        d, first, n = parts[r]
        other = lax.rem(at.p + n_pb - d, n_pb)
        ref = c_all.at[pl.ds(pl.multiple_of(other * half + first, n), n)]
        remote(ref, ref, c_send.at[r], c_recv.at[r], at.dev(at.me)).wait_recv()

    own_q.wait()
    forward(0, 0, True)
    own_c.wait()
    for r in range(n_far):
        c_copy(r).start()

    assert cols % LANES == 0 and cols // 8 < 256 and tall % group == 0
    for h, copy in zip(range(0, tall, group), g_copies):
        copy.wait()

        def turn(k, codes, h=h):
            cc = span(k, LANES)
            word = g_raw[h : h + LANES, cc]
            for i in range(1, 8):
                word = word + jnp.left_shift(g_raw[h + i * LANES : h + (i + 1) * LANES, cc], 3 * i)
            word = word.T
            new = []
            for i in range(8):
                g = jnp.right_shift(word, 3 * i) & 7
                g_all[cc, h + i * LANES : h + (i + 1) * LANES] = g
                one = jnp.left_shift(1, g * 8)
                code = codes[i]
                for j in range(0, LANES, 8):
                    code = code + one[j : j + 8]
                new.append(code)
            return tuple(new)

        codes = lax.fori_loop(
            0, cols // LANES, turn, tuple(jnp.zeros((8, LANES), jnp.int32) for _ in range(8))
        )
        for i in range(8):
            for b in range(G - 1):
                field = (jnp.right_shift(codes[i], 8 * b) & 255).astype(F32)
                counts[b : b + 1, h + i * LANES : h + (i + 1) * LANES] = jnp.sum(field, axis=0, keepdims=True)

    def score(chip, wide, start, size, part):
        cc = pl.ds(pl.multiple_of(start, size), size)
        s = lax.dot_general(
            c_all[cc], q_all[pl.ds(pl.multiple_of(chip * pair, wide), wide)],
            (((1,), (1,)), ((), ())), preferred_element_type=F32,
        ) * (scaling * LOG2E)
        for x in range(0, wide, LANES):
            qq = pl.ds(pl.multiple_of(chip * pair + x, LANES), LANES)
            tile = s[:, x : x + LANES]
            s_all[cc, qq] = tile

            def put(i, row):
                tables[chip + x // pair, part, i : i + 1, x % pair : x % pair + LANES] = row

            statistics(tile, g_all[cc, qq], put)

    def near(k, dm):
        score(at.chip(at.visit(k), dm), pair, at.p * half, half, 0)

    def far(k, r):
        d, first, n = parts[r]
        score(2 * at.visit(k), quad, lax.rem(at.p + n_pb - d, n_pb) * half + first, n, r + 1)

    def stat_copy(block):
        return remote(stats.at[block], got.at[at.me], s_send.at[block], s_recv.at[at.me], at.dev(block))

    def join(k):
        for m in range(2):
            chip = 2 * at.visit(k) + m
            tabs = [tables[chip, h] for h in range(n_far + 1)]
            top = tabs[0][:G]
            for tab in tabs[1:]:
                top = jnp.maximum(top, tab[:G])
            mass = jnp.zeros_like(top)
            total = jnp.zeros((1, pair), F32)
            for tab in tabs:
                upto = tab[G : 2 * G]
                own = jnp.concatenate([upto[:1], upto[1:] - upto[:-1]], axis=0)
                mass = mass + own * jnp.exp2(tab[:G] - top)
                total = total + tab[2 * G : 2 * G + 1]
            count = counts[:, span(chip, pair)][: G - 1]
            whole = jnp.concatenate([top, mass, total, count, jnp.zeros((1, pair), F32)], axis=0)
            for c in range(2):
                block = chip * 2 + c
                stats[block] = whole[:, c * rows : (c + 1) * rows]

                @pl.when(block != at.me)
                def _():
                    stat_copy(block).start()

    partner(0, 0)

    def step(u, carry):
        @pl.when(u > 0)
        def _():
            forward(u, 0, True)
            forward(u - 1, 1, True)
            partner(u - 1, 1)
            near(u - 1, 1)
            partner(u, 0)

        near(u, 0)

        @pl.when(u == 2)
        def _():
            for r in range(early):
                c_arrived(r)

        @pl.when(u >= 2)
        def _():
            for r in range(early):
                far(u - 2, r)

        return carry

    lax.fori_loop(0, outs, step, 0)
    if outs < 3:
        for r in range(early):
            c_arrived(r)
    for k in range(max(outs - 2, 0), outs - 1):
        for r in range(early):
            far(k, r)
    for r in range(early, n_far):
        c_arrived(r)

        def body(k, carry, r=r):
            far(k, r)
            return carry

        lax.fori_loop(0, outs - 1, body, 0)

    def joins(k, carry):
        join(k)
        return carry

    lax.fori_loop(0, outs - 1, joins, 0)
    forward(outs - 1, 1, True)
    partner(outs - 1, 1)
    near(outs - 1, 1)
    for r in range(n_far):
        far(outs - 1, r)
    join(outs - 1)

    others = [lax.rem(at.me + d, n_col) for d in range(1, n_col)]
    got[at.me] = stats[at.me]
    for o in others:
        remote(stats.at[o], got.at[o], s_send.at[o], s_recv.at[o], at.dev(at.me)).wait_recv()
    mine[...] = finish(got, n_col, cols, columns)

    def merged_copy(o):
        return remote(mine, merged.at[at.me], m_send.at[o], m_recv.at[at.me], at.dev(o))

    for o in others:
        merged_copy(o).start()
    merged[at.me] = mine[...]
    for o in others:
        remote(mine, merged.at[o], m_send.at[o], m_recv.at[o], at.dev(at.me)).wait_recv()

    chunk = min(LANES, half)

    def slope(chip, start, size):
        qq = span(chip, pair)
        table = jnp.concatenate([merged[2 * chip], merged[2 * chip + 1]], axis=1)
        w = w_ref[pl.ds(chip, 1), :]
        loss_ref[pl.ds(chip, 1), :] = table[G : G + 1]

        def body(j, carry):
            cc = pl.ds(pl.multiple_of(start + j * chunk, chunk), chunk)
            g = g_all[cc, qq]
            off = jnp.broadcast_to(table[G - 1 : G], g.shape)
            for b in range(G - 2, -1, -1):
                off = jnp.where(g <= b, table[b : b + 1], off)
            slopes[cc, qq] = (w * jnp.exp2(s_all[cc, qq] + off) - w).astype(BF16)
            return carry

        if size == chunk:
            body(0, 0)
        else:
            lax.fori_loop(0, size // chunk, body, 0)

    def k_copy(chip):
        return remote(
            q_part.at[chip, lax.rem(at.core + 1, 2)], core_got.at[chip], k_send.at[chip], k_recv.at[chip],
            at.dev(at.block(at.out, 0, 1)),
        )

    def q_grad(t):
        out, dm = at.item(t)
        chip = at.chip(out, dm)
        part = lax.dot_general(
            slopes[:, span(chip, pair)], c_all[...], (((0,), (0,)), ((), ())), preferred_element_type=F32
        ) * scaling
        q_part[chip] = part.astype(BF16).reshape(2, rows, width)
        k_copy(chip).start()

    def sub_rows(s):
        return pl.ds(s * sub, sub)

    def y_copy(out, s):
        return remote(
            q_part.at[at.chip(out, 1), at.core, sub_rows(s)], y_got.at[out, sub_rows(s)],
            y_send.at[out, s], y_recv.at[out, s], at.dev(at.block(at.out, 1, 0)),
        )

    def cross(out):
        chip = at.chip(out, 1)
        k_copy(chip).wait_recv()
        for s in range(SUBS):
            rr = sub_rows(s)
            both = q_part[chip, at.core, rr].astype(F32) + core_got[chip, rr].astype(F32)
            q_part[chip, at.core, rr] = both.astype(BF16)
            y_copy(out, s).start()

    def z_copy(out, s):
        toward = jnp.where(out > at.out, at.out + 1, at.out - 1)
        slot = jnp.where((out < at.out) & (toward == out), outs, out)
        return remote(
            z_part.at[out, sub_rows(s)], z_got.at[slot, sub_rows(s)],
            z_send.at[out, s], z_recv.at[slot, s], at.dev(at.block(toward, 0, 0)),
        )

    def z_add(slot, s):
        ref = z_got.at[slot, sub_rows(s)]
        remote(ref, ref, z_send.at[0, s], z_recv.at[slot, s], at.dev(at.me)).wait_recv()
        acc[...] += z_got[slot, sub_rows(s)].astype(F32)

    def gather_row(out, s):
        chip = at.chip(out, 0)
        rr = sub_rows(s)
        ref = y_got.at[out, rr]
        remote(ref, ref, y_send.at[out, s], y_recv.at[out, s], at.dev(at.me)).wait_recv()
        acc[...] = (
            q_part[chip, at.core, rr].astype(F32)
            + core_got[chip, rr].astype(F32)
            + y_got[out, rr].astype(F32)
        )

    def chain(v):
        out = at.visit(v)
        k_copy(at.chip(out, 0)).wait_recv()
        behind = ((out > at.out) & (at.out > 0)) | ((out < at.out) & (at.out < outs - 1))
        for s in range(SUBS):
            gather_row(out, s)

            @pl.when(behind)
            def _():
                z_add(out, s)

            z_part[out, sub_rows(s)] = acc[...].astype(BF16)
            z_copy(out, s).start()

    per = half // chunk
    n_x = per * (n_pb - 1)

    def x_copy(r):
        d, j = 1 + r // per, lax.rem(r, per)
        other = lax.rem(at.p + d, n_pb)
        rr = pl.ds(pl.multiple_of(j * chunk, chunk), chunk)
        return remote(
            c_part.at[r], c_got.at[d - 1, rr], x_send.at[r], x_recv.at[r], {"pb": other, "col": at.me}
        )

    def c_grad(start):
        here = slopes[pl.ds(pl.multiple_of(start, chunk), chunk), :]
        return jnp.dot(here, q_all[...], preferred_element_type=F32) * scaling

    def c_far(r):
        other = lax.rem(at.p + 1 + r // per, n_pb)
        c_part[r] = c_grad(other * half + lax.rem(r, per) * chunk).astype(BF16)
        x_copy(r).start()

    def slope_first(i, carry):
        slope(i, lax.rem(at.p + 1, n_pb) * half, chunk)
        return carry

    def slope_step(i, carry):
        out, dm = at.item(i)
        slope(at.chip(out, dm), 0, cols)

        @pl.when(i == 0)
        def _():
            q_grad(0)

        @pl.when(i == 2)
        def _():
            cross(at.visit(outs - 1))

        return carry

    lax.fori_loop(0, chips, slope_first, 0)
    c_far(0)
    lax.fori_loop(0, chips, slope_step, 0)

    def grad_step(j, carry):
        @pl.when((j > 0) & (j < n_x))
        def _():
            c_far(j)

        @pl.when(j + 1 < chips)
        def _():
            q_grad(j + 1)

        @pl.when((j >= 1) & (lax.rem(j, 2) == 1) & (j < chips - 1))
        def _():
            cross(at.item(j)[0])

        return carry

    lax.fori_loop(0, max(n_x, chips - 1), grad_step, 0)

    def c_near(j, carry):
        c_own[pl.ds(pl.multiple_of(j * chunk, chunk), chunk)] = c_grad(at.p * half + j * chunk)
        return carry

    def chain_step(i, carry):
        chain(outs - 1 - i)

        @pl.when(i == 0)
        def _():
            lax.fori_loop(0, per, c_near, 0)

        return carry

    lax.fori_loop(0, outs - 1, chain_step, 0)
    k_copy(at.chip(at.out, 0)).wait_recv()
    for s in range(SUBS):
        gather_row(at.out, s)

        @pl.when(at.out > 0)
        def _():
            z_add(at.out, s)

        @pl.when(at.out < outs - 1)
        def _():
            z_add(outs, s)

        q_out[sub_rows(s), :] = acc[...].astype(BF16)

    def c_finish(j, carry):
        rr = pl.ds(pl.multiple_of(j * chunk, chunk), chunk)
        total = c_own[rr]
        for d in range(1, n_pb):
            r = (d - 1) * per + j
            ref = c_got.at[d - 1, rr]
            remote(ref, ref, x_send.at[r], x_recv.at[r], at.dev(at.me)).wait_recv()
            total = total + c_got[d - 1, rr].astype(F32)
        c_out[rr] = total.astype(BF16)
        return carry

    lax.fori_loop(0, per, c_finish, 0)

    def drain(k, carry):
        for dm in range(2):
            forward(k, dm, False)
        out = at.visit(k)
        for dm in range(2):
            k_copy(at.chip(out, dm)).wait_send()
        for s in range(SUBS):
            y_copy(out, s).wait_send()

            @pl.when(k > 0)
            def _():
                z_copy(out, s).wait_send()

        return carry

    lax.fori_loop(0, outs, drain, 0)
    for r in range(n_far):
        c_copy(r).wait_send()
    for o in others:
        stat_copy(o).wait_send()
        merged_copy(o).wait_send()
    lax.fori_loop(0, n_x, lambda r, c: (x_copy(r).wait_send(), c)[1], 0)


def local(queries, candidates, grades, query_weights):
    n_col, n_pb = lax.axis_size("col"), lax.axis_size("pb")
    rows, width = queries.shape
    half = candidates.shape[0]
    tall, cols = grades.shape
    scaling = 1.0 / math.sqrt(width)
    n_far = len(far_parts_of(half, n_pb))
    outs, chips = n_col // 4, n_col // 2
    chunk = min(LANES, half)
    n_x = half // chunk * (n_pb - 1)
    sub = rows // SUBS
    dma = pltpu.SemaphoreType.DMA
    vmem = pl.BlockSpec(memory_space=pltpu.VMEM)
    hbm = pl.BlockSpec(memory_space=pl.ANY)
    losses, query_grad, cand_grad = pl.pallas_call(
        functools.partial(kernel, n_col, n_pb, scaling, cols * n_col),
        out_shape=(
            jax.ShapeDtypeStruct((chips, 2 * rows), F32),
            jax.ShapeDtypeStruct((rows, width), BF16),
            jax.ShapeDtypeStruct((half, width), BF16),
        ),
        in_specs=[hbm, hbm, hbm, vmem],
        out_specs=(vmem, vmem, vmem),
        scratch_shapes=[
            pltpu.VMEM((tall, width), BF16),
            pltpu.VMEM((cols, width), BF16),
            pltpu.VMEM((tall, cols), jnp.int32),
            pltpu.VMEM((cols, tall), jnp.int32),
            pltpu.VMEM((cols, tall), F32),
            pltpu.VMEM((cols, tall), BF16),
            pltpu.VMEM((chips, 1 + n_far, STATS, 2 * rows), F32),
            pltpu.VMEM((8, tall), F32),
            pltpu.VMEM((n_col, STATS, rows), F32),
            pltpu.VMEM((n_col, STATS, rows), F32),
            pltpu.VMEM((8, rows), F32),
            pltpu.VMEM((n_col, 8, rows), F32),
            pltpu.VMEM((chips, 2, rows, width), BF16),
            pltpu.VMEM((chips, rows, width), BF16),
            pltpu.VMEM((outs, rows, width), BF16),
            pltpu.VMEM((outs + 1, rows, width), BF16),
            pltpu.VMEM((outs, rows, width), BF16),
            pltpu.VMEM((sub, width), F32),
            pltpu.VMEM((n_x, chunk, width), BF16),
            pltpu.VMEM((half, width), F32),
            pltpu.VMEM((n_pb - 1, half, width), BF16),
            dma((2,)),
            dma((tall // (8 * LANES),)),
            dma((n_col, 4, SUBS)),
            dma((n_col, SUBS)),
            dma((n_far,)),
            dma((n_far,)),
            dma((n_col,)),
            dma((n_col,)),
            dma((n_col,)),
            dma((n_col,)),
            dma((chips,)),
            dma((chips,)),
            dma((outs, SUBS)),
            dma((outs, SUBS)),
            dma((outs, SUBS)),
            dma((outs + 1, SUBS)),
            dma((n_x,)),
            dma((n_x,)),
        ],
        compiler_params=pltpu.CompilerParams(
            collective_id=0, has_side_effects=True, vmem_limit_bytes=62 * 2**20
        ),
        name="listmle",
    )(queries, candidates, grades, query_weights.reshape(chips, 2 * rows))
    return (losses.reshape(-1), query_grad, cand_grad)


def solution(mesh):
    in_specs = (P(("pb", "col"), None), P(("col", "pb"), None), P("pb", "col"), P("pb"))
    out_specs = (P("pb"), P(("pb", "col"), None), P(("col", "pb"), None))
    return jax.shard_map(local, mesh=mesh, in_specs=in_specs, out_specs=out_specs, check_vma=False)
```

```python
import functools
import math

import jax
import jax.numpy as jnp
from jax import lax
from jax.experimental import pallas as pl
from jax.experimental.pallas import tpu as pltpu
from jax.sharding import PartitionSpec as P

GRADES = 5
STATS = 16
COUNT_ROWS = (5, 6, 7, 14)
LOWEST = -1e30
LANES = 128
SUBS = 2
MESH = pl.DeviceIdType.MESH
F32 = jnp.float32
BF16 = jnp.bfloat16
LOG2E = math.log2(math.e)
LN2 = math.log(2.0)


class Place:
    def __init__(self, n_col, n_pb):
        assert n_col % 4 == 0
        self.n_col, self.n_pb = n_col, n_pb
        self.cores = self.mids = 2
        self.chips = n_col // 2
        self.outs = n_col // 4
        self.me = lax.axis_index("col")
        self.p = lax.axis_index("pb")
        self.core = lax.rem(self.me, 2)
        self.mid = lax.rem(self.me // 2, 2)
        self.out = self.me // 4

    def chip(self, out, dm):
        return out * 2 + lax.rem(self.mid + dm, 2)

    def block(self, out, dm, dc):
        return self.chip(out, dm) * 2 + lax.rem(self.core + dc, 2)

    def dev(self, col):
        return {"pb": self.p, "col": col}

    def visit(self, k):
        side = jnp.minimum(self.out, self.outs - 1 - self.out)
        near = (k + 1) // 2 * (2 * lax.rem(k, 2) - 1)
        far = (k - side) * jnp.where(2 * self.out < self.outs, 1, -1)
        return self.out + jnp.where(k <= 2 * side, near, far)

    def item(self, t):
        odd = (lax.rem(t, 2) == 1) & (t < self.chips - 1)
        first = t == 0
        v = jnp.where(odd, self.outs - 1 - (t + 1) // 2, self.outs - 1 - (t - 1) // 2)
        v = jnp.where(first, self.outs - 1, v)
        dm = jnp.where(odd | first, 1, 0)
        return self.visit(v), dm


def remote(src, dst, send, recv, device):
    return pltpu.make_async_remote_copy(
        src_ref=src, dst_ref=dst, send_sem=send, recv_sem=recv, device_id=device, device_id_type=MESH
    )


def span(block, size):
    return pl.ds(pl.multiple_of(block * size, size), size)


def statistics(s, g, put):
    tops = [jnp.max(jnp.where(g <= b, s, LOWEST), axis=0, keepdims=True) for b in range(GRADES - 1)]
    tops.append(jnp.max(s, axis=0, keepdims=True))
    picked = jnp.broadcast_to(tops[-1], s.shape)
    for b in range(GRADES - 2, -1, -1):
        picked = jnp.where(g <= b, tops[b], picked)
    e = jnp.exp2(s - picked)
    sums = [jnp.sum(jnp.where(g <= b, e, 0.0), axis=0, keepdims=True) for b in range(GRADES - 1)]
    sums.append(jnp.sum(e, axis=0, keepdims=True))
    for b in range(GRADES):
        put(b, tops[b])
        put(8 + b, sums[b] - sums[b - 1] if b else sums[b])
    put(8 + GRADES, jnp.sum(s, axis=0, keepdims=True))


def finish(got, n_col, cols, columns):
    G = GRADES
    rows = got.shape[2]
    graded = lax.broadcasted_iota(jnp.int32, (8, rows), 0) < G
    tops = got[0][:8]
    first = jnp.zeros_like(tops)
    for k in range(1, n_col):
        tops = jnp.maximum(tops, got[k][:8])
    second = first
    for k in range(n_col):
        block = got[k]
        first = first + block[:8]
        second = second + block[8:] * jnp.where(graded, jnp.exp2(block[:8] - tops), 1.0)
    top = [tops[b : b + 1] for b in range(G)]
    mass = [second[b : b + 1] for b in range(G)]
    total = second[G : G + 1]
    both = jnp.concatenate([first, second], axis=0)
    count = [both[r : r + 1] for r in COUNT_ROWS]
    count.append(float(cols * n_col) - (count[0] + count[1] + count[2] + count[3]))
    levels = []
    seen = jnp.zeros_like(total)
    summed = seen
    weighted = seen
    for b in range(G):
        seen = seen + count[b]
        summed = mass[b] if b == 0 else mass[b] + summed * jnp.exp2(top[b - 1] - top[b])
        present = seen > 0.0
        level = jnp.where(present, top[b] + jnp.log(jnp.where(present, summed, 1.0)) * LOG2E, top[b])
        levels.append(level)
        weighted = weighted + count[b] * level
    loss = (weighted - total) * (LN2 / columns)
    offsets = [None] * G
    factor = seen * 0.0
    for b in range(G - 1, -1, -1):
        own = count[b] * jnp.exp2(top[b] - levels[b])
        factor = own if b == G - 1 else own + factor * jnp.exp2(top[b] - top[b + 1])
        offsets[b] = jnp.log(jnp.maximum(factor, 1e-37)) * LOG2E - top[b]
    pad = jnp.zeros((8 - G - 1, loss.shape[1]), F32)
    return jnp.concatenate(offsets + [loss, pad], axis=0)


def far_parts_of(half, n_pb):
    sizes = [half // 2, half // 4, half // 4] if half % 512 == 0 else [half]
    return [(d, sum(sizes[:i]), n) for i, n in enumerate(sizes) for d in range(1, n_pb)]


def kernel(
    n_col, n_pb, scaling, columns,
    q_hbm, c_hbm, g_hbm, w_ref, loss_ref, q_out, c_out,
    q_all, c_all, g_raw, g_all, s_all, slopes, tables, counts, stats, got, mine, merged,
    q_part, core_got, y_got, z_got, z_part, acc, c_part, c_own, c_got,
    own_sem, g_sem, q_send, q_recv, c_send, c_recv, s_send, s_recv, m_send, m_recv,
    k_send, k_recv, y_send, y_recv, z_send, z_recv, x_send, x_recv,
):
    at = Place(n_col, n_pb)
    rows, width = q_hbm.shape
    half = c_hbm.shape[0]
    tall, cols = g_hbm.shape
    pair, quad = 2 * rows, 4 * rows
    sub = rows // SUBS
    outs, chips = at.outs, at.chips
    G = GRADES
    parts = far_parts_of(half, n_pb)
    n_far = len(parts)
    early = n_pb - 1

    own_q = pltpu.make_async_copy(q_hbm, q_all.at[span(at.me, rows)], own_sem.at[0])
    own_c = pltpu.make_async_copy(c_hbm, c_all.at[span(at.p, half)], own_sem.at[1])
    own_q.start()
    own_c.start()
    group = 8 * LANES
    g_copies = [
        pltpu.make_async_copy(g_hbm.at[pl.ds(h, group)], g_raw.at[pl.ds(h, group)], g_sem.at[h // group])
        for h in range(0, tall, group)
    ]
    for copy in g_copies:
        copy.start()
    barrier = pltpu.get_barrier_semaphore()
    for d in range(1, n_col):
        pl.semaphore_signal(
            barrier, inc=1, device_id=at.dev(lax.rem(at.me + d, n_col)), device_id_type=MESH
        )
    for d in range(1, n_pb):
        pl.semaphore_signal(
            barrier, inc=1, device_id={"pb": lax.rem(at.p + d, n_pb), "col": at.me}, device_id_type=MESH
        )
    pl.semaphore_wait(barrier, n_col + n_pb - 2)

    def q_span(block, s):
        return pl.ds(pl.multiple_of(block * rows + s * sub, sub), sub)

    def q_copy(block, s, t, col):
        ref = q_all.at[q_span(block, s)]
        return remote(ref, ref, q_send.at[block, t, s], q_recv.at[block, s], at.dev(col))

    def forward(k, dm, act, subs=range(SUBS)):
        out = at.visit(k)
        block = at.block(out, dm, 0)
        for s in subs:
            if act and not (isinstance(k, int) and k == 0 and dm == 0):
                q_copy(block, s, 0, at.me).wait_recv()

            def go(t, col):
                copy = q_copy(block, s, t, col)
                copy.start() if act else copy.wait_send()

            if dm == 0:
                @pl.when((out <= at.out) & (at.out < outs - 1))
                def _():
                    go(0, at.block(at.out + 1, 0, 0))

                @pl.when((out >= at.out) & (at.out > 0))
                def _():
                    go(1, at.block(at.out - 1, 0, 0))

                go(2, at.block(at.out, 1, 0))
            go(3, at.block(at.out, 0, 1))

    def partner(k, dm):
        block = at.block(at.visit(k), dm, 1)
        for s in range(SUBS):
            q_copy(block, s, 0, at.me).wait_recv()

    def c_copy(r):
        d, first, n = parts[r]
        ref = c_all.at[pl.ds(pl.multiple_of(at.p * half + first, n), n)]
        other = lax.rem(at.p + d, n_pb)
        return remote(ref, ref, c_send.at[r], c_recv.at[r], {"pb": other, "col": at.me})

    def c_arrived(r):
        d, first, n = parts[r]
        other = lax.rem(at.p + n_pb - d, n_pb)
        ref = c_all.at[pl.ds(pl.multiple_of(other * half + first, n), n)]
        remote(ref, ref, c_send.at[r], c_recv.at[r], at.dev(at.me)).wait_recv()

    own_q.wait()
    forward(0, 0, True)
    counts[...] = jnp.zeros(counts.shape, F32)

    def clear(chip, carry):
        for h in range(n_far + 1):
            tables[chip, h] = jnp.zeros((STATS, pair), F32)
        return carry

    lax.fori_loop(0, chips, clear, 0)
    own_c.wait()
    for r in range(n_far):
        c_copy(r).start()

    assert cols % LANES == 0 and cols // 8 < 256 and tall % group == 0
    for h, copy in zip(range(0, tall, group), g_copies):
        copy.wait()

        def turn(k, codes, h=h):
            cc = span(k, LANES)
            word = g_raw[h : h + LANES, cc]
            for i in range(1, 8):
                word = word + jnp.left_shift(g_raw[h + i * LANES : h + (i + 1) * LANES, cc], 3 * i)
            word = word.T
            new = []
            for i in range(8):
                g = jnp.right_shift(word, 3 * i) & 7
                g_all[cc, h + i * LANES : h + (i + 1) * LANES] = g
                one = jnp.left_shift(1, g * 8)
                code = codes[i]
                for j in range(0, LANES, 8):
                    code = code + one[j : j + 8]
                new.append(code)
            return tuple(new)

        codes = lax.fori_loop(
            0, cols // LANES, turn, tuple(jnp.zeros((8, LANES), jnp.int32) for _ in range(8))
        )
        for i in range(8):
            for b in range(G - 1):
                field = (jnp.right_shift(codes[i], 8 * b) & 255).astype(F32)
                row = COUNT_ROWS[b]
                counts[row : row + 1, h + i * LANES : h + (i + 1) * LANES] = jnp.sum(field, axis=0, keepdims=True)

    def score(chip, wide, start, size, part):
        cc = pl.ds(pl.multiple_of(start, size), size)
        s = lax.dot_general(
            c_all[cc], q_all[pl.ds(pl.multiple_of(chip * pair, wide), wide)],
            (((1,), (1,)), ((), ())), preferred_element_type=F32,
        ) * (scaling * LOG2E)
        for x in range(0, wide, LANES):
            qq = pl.ds(pl.multiple_of(chip * pair + x, LANES), LANES)
            tile = s[:, x : x + LANES]
            s_all[cc, qq] = tile

            def put(i, row):
                tables[chip + x // pair, part, i : i + 1, x % pair : x % pair + LANES] = row

            statistics(tile, g_all[cc, qq], put)

    def near(k, dm):
        score(at.chip(at.visit(k), dm), pair, at.p * half, half, 0)

    def far(k, r, dm=None):
        d, first, n = parts[r]
        chip, wide = (2 * at.visit(k), quad) if dm is None else (at.chip(at.visit(k), dm), pair)
        score(chip, wide, lax.rem(at.p + n_pb - d, n_pb) * half + first, n, r + 1)

    def stat_copy(block):
        return remote(stats.at[block], got.at[at.me], s_send.at[block], s_recv.at[at.me], at.dev(block))

    def join(ks):
        todo = [2 * at.visit(k) + m for k in ks for m in range(2)]
        for chip in todo:
            tabs = [tables[chip, h] for h in range(n_far + 1)]
            top = tabs[0][:8]
            for tab in tabs[1:]:
                top = jnp.maximum(top, tab[:8])
            mass = sum(tab[8:] * jnp.exp2(tab[:8] - top) for tab in tabs)
            count = counts[:, span(chip, pair)]
            for c in range(2):
                here = slice(c * rows, (c + 1) * rows)
                stats[chip * 2 + c, :8] = (top + count[:8])[:, here]
                stats[chip * 2 + c, 8:] = (mass + count[8:])[:, here]
        for chip in todo:
            for c in range(2):
                @pl.when(chip * 2 + c != at.me)
                def _():
                    stat_copy(chip * 2 + c).start()

    partner(0, 0)
    near(0, 0)
    if outs > 1:
        forward(1, 0, True, [0])

    def step(u, carry):
        forward(u, 0, True, range(1, SUBS))
        forward(u - 1, 1, True)
        partner(u - 1, 1)
        near(u - 1, 1)

        @pl.when(u + 1 < outs)
        def _():
            forward(u + 1, 0, True, [0])

        partner(u, 0)
        near(u, 0)

        @pl.when(u == 2)
        def _():
            for r in range(early):
                c_arrived(r)

        @pl.when(u >= 2)
        def _():
            for r in range(early):
                far(u - 2, r)

        return carry

    lax.fori_loop(1, outs, step, 0)
    if outs < 3:
        for r in range(early):
            c_arrived(r)
    for k in range(max(outs - 2, 0), outs - 1):
        for r in range(early):
            far(k, r)
    for r in range(n_far):
        if r >= early:
            c_arrived(r)

            def body(k, carry, r=r):
                far(k, r)
                return carry

            lax.fori_loop(0, outs - 1, body, 0)
        far(outs - 1, r, 0)

    forward(outs - 1, 1, True)

    join(range(outs - 1))
    partner(outs - 1, 1)
    near(outs - 1, 1)
    for r in range(n_far):
        far(outs - 1, r, 1)
    join([outs - 1])

    others = [lax.rem(at.me + d, n_col) for d in range(1, n_col)]
    got[at.me] = stats[at.me]
    for o in others:
        remote(stats.at[o], got.at[o], s_send.at[o], s_recv.at[o], at.dev(at.me)).wait_recv()
    mine[...] = finish(got, n_col, cols, columns)

    def merged_copy(o):
        return remote(mine, merged.at[at.me], m_send.at[o], m_recv.at[at.me], at.dev(o))

    for o in others:
        merged_copy(o).start()
    merged[at.me] = mine[...]
    for o in others:
        remote(mine, merged.at[o], m_send.at[o], m_recv.at[o], at.dev(at.me)).wait_recv()

    chunk = min(LANES, half)

    def slope(chip, start, size):
        qq = span(chip, pair)
        table = jnp.concatenate([merged[2 * chip], merged[2 * chip + 1]], axis=1)
        few = pair // LANES
        w = [w_ref[pl.ds(chip * few + x, 1), :] for x in range(few)]
        w = jnp.concatenate(w, axis=1)
        for x in range(0, pair, LANES):
            loss_ref[pl.ds(chip * (pair // LANES) + x // LANES, 1), :] = table[G : G + 1, x : x + LANES]

        def body(j, carry):
            cc = pl.ds(pl.multiple_of(start + j * chunk, chunk), chunk)
            g = g_all[cc, qq]
            off = jnp.broadcast_to(table[G - 1 : G], g.shape)
            for b in range(G - 2, -1, -1):
                off = jnp.where(g <= b, table[b : b + 1], off)
            slopes[cc, qq] = (w * jnp.exp2(s_all[cc, qq] + off) - w).astype(BF16)
            return carry

        if size == chunk:
            body(0, 0)
        else:
            lax.fori_loop(0, size // chunk, body, 0)

    def k_copy(chip):
        return remote(
            q_part.at[chip, lax.rem(at.core + 1, 2)], core_got.at[chip], k_send.at[chip], k_recv.at[chip],
            at.dev(at.block(at.out, 0, 1)),
        )

    def q_grad(t):
        out, dm = at.item(t)
        chip = at.chip(out, dm)
        part = lax.dot_general(
            slopes[:, span(chip, pair)], c_all[...], (((0,), (0,)), ((), ())), preferred_element_type=F32
        ) * scaling
        q_part[chip] = part.astype(BF16).reshape(2, rows, width)
        k_copy(chip).start()

    def sub_rows(s):
        return pl.ds(s * sub, sub)

    def y_copy(out, s):
        return remote(
            q_part.at[at.chip(out, 1), at.core, sub_rows(s)], y_got.at[out, sub_rows(s)],
            y_send.at[out, s], y_recv.at[out, s], at.dev(at.block(at.out, 1, 0)),
        )

    def cross(out):
        chip = at.chip(out, 1)
        k_copy(chip).wait_recv()
        for s in range(SUBS):
            rr = sub_rows(s)
            both = q_part[chip, at.core, rr].astype(F32) + core_got[chip, rr].astype(F32)
            q_part[chip, at.core, rr] = both.astype(BF16)
            y_copy(out, s).start()

    def z_copy(out, s):
        toward = jnp.where(out > at.out, at.out + 1, at.out - 1)
        slot = jnp.where((out < at.out) & (toward == out), outs, out)
        return remote(
            z_part.at[out, sub_rows(s)], z_got.at[slot, sub_rows(s)],
            z_send.at[out, s], z_recv.at[slot, s], at.dev(at.block(toward, 0, 0)),
        )

    def z_add(slot, s):
        ref = z_got.at[slot, sub_rows(s)]
        remote(ref, ref, z_send.at[0, s], z_recv.at[slot, s], at.dev(at.me)).wait_recv()
        acc[...] += z_got[slot, sub_rows(s)].astype(F32)

    def gather_row(out, s):
        chip = at.chip(out, 0)
        rr = sub_rows(s)
        ref = y_got.at[out, rr]
        remote(ref, ref, y_send.at[out, s], y_recv.at[out, s], at.dev(at.me)).wait_recv()
        acc[...] = (
            q_part[chip, at.core, rr].astype(F32)
            + core_got[chip, rr].astype(F32)
            + y_got[out, rr].astype(F32)
        )

    def chain(v):
        out = at.visit(v)
        k_copy(at.chip(out, 0)).wait_recv()
        behind = ((out > at.out) & (at.out > 0)) | ((out < at.out) & (at.out < outs - 1))
        for s in range(SUBS):
            gather_row(out, s)

            @pl.when(behind)
            def _():
                z_add(out, s)

            z_part[out, sub_rows(s)] = acc[...].astype(BF16)
            z_copy(out, s).start()

    per = half // chunk
    n_x = per * (n_pb - 1)

    def x_copy(r):
        d, j = 1 + r // per, lax.rem(r, per)
        other = lax.rem(at.p + d, n_pb)
        rr = pl.ds(pl.multiple_of(j * chunk, chunk), chunk)
        return remote(
            c_part.at[r], c_got.at[d - 1, rr], x_send.at[r], x_recv.at[r], {"pb": other, "col": at.me}
        )

    def c_grad(start):
        here = slopes[pl.ds(pl.multiple_of(start, chunk), chunk), :]
        return jnp.dot(here, q_all[...], preferred_element_type=F32) * scaling

    def c_far(r):
        other = lax.rem(at.p + 1 + r // per, n_pb)
        c_part[r] = c_grad(other * half + lax.rem(r, per) * chunk).astype(BF16)
        x_copy(r).start()

    def slope_first(i, carry):
        slope(i, lax.rem(at.p + 1, n_pb) * half, chunk)
        return carry

    def slope_step(i, carry):
        out, dm = at.item(i)
        slope(at.chip(out, dm), 0, cols)

        @pl.when(i == 0)
        def _():
            q_grad(0)

        @pl.when(i == 2)
        def _():
            cross(at.visit(outs - 1))

        return carry

    lax.fori_loop(0, chips, slope_first, 0)
    c_far(0)
    lax.fori_loop(0, chips, slope_step, 0)

    edge = (at.out == 0) | (at.out == outs - 1)

    def grad_step(j, carry):
        @pl.when((j > 0) & (j < n_x))
        def _():
            c_far(j)

        @pl.when(j + 1 < chips)
        def _():
            q_grad(j + 1)

        @pl.when((j >= 1) & (lax.rem(j, 2) == 1) & (j < chips - 1))
        def _():
            cross(at.item(j)[0])

        @pl.when((j == 2) & edge)
        def _():
            chain(outs - 1)

        return carry

    lax.fori_loop(0, max(n_x, chips - 1), grad_step, 0)

    def c_near(j, carry):
        c_own[pl.ds(pl.multiple_of(j * chunk, chunk), chunk)] = c_grad(at.p * half + j * chunk)
        return carry

    def chain_step(i, carry):
        @pl.when((i > 0) | jnp.logical_not(edge))
        def _():
            chain(outs - 1 - i)

        @pl.when(i == min(1, outs - 2))
        def _():
            lax.fori_loop(0, per, c_near, 0)

        return carry

    lax.fori_loop(0, outs - 1, chain_step, 0)
    k_copy(at.chip(at.out, 0)).wait_recv()
    for s in range(SUBS):
        gather_row(at.out, s)

        @pl.when(at.out > 0)
        def _():
            z_add(at.out, s)

        @pl.when(at.out < outs - 1)
        def _():
            z_add(outs, s)

        q_out[sub_rows(s), :] = acc[...].astype(BF16)

    def c_finish(j, carry):
        rr = pl.ds(pl.multiple_of(j * chunk, chunk), chunk)
        total = c_own[rr]
        for d in range(1, n_pb):
            r = (d - 1) * per + j
            ref = c_got.at[d - 1, rr]
            remote(ref, ref, x_send.at[r], x_recv.at[r], at.dev(at.me)).wait_recv()
            total = total + c_got[d - 1, rr].astype(F32)
        c_out[rr] = total.astype(BF16)
        return carry

    lax.fori_loop(0, per, c_finish, 0)

    def drain(k, carry):
        for dm in range(2):
            forward(k, dm, False)
        out = at.visit(k)
        for dm in range(2):
            k_copy(at.chip(out, dm)).wait_send()
        for s in range(SUBS):
            y_copy(out, s).wait_send()

            @pl.when(k > 0)
            def _():
                z_copy(out, s).wait_send()

        return carry

    lax.fori_loop(0, outs, drain, 0)
    for r in range(n_far):
        c_copy(r).wait_send()
    for o in others:
        stat_copy(o).wait_send()
        merged_copy(o).wait_send()
    lax.fori_loop(0, n_x, lambda r, c: (x_copy(r).wait_send(), c)[1], 0)


def copy_kernel(*refs):
    n = (len(refs) - 2) // 3
    sources, outs, held = refs[:n], refs[n : 2 * n], refs[2 * n : 3 * n]
    into, back = refs[3 * n :]
    reads = [pltpu.make_async_copy(a, h, into.at[i]) for i, (a, h) in enumerate(zip(sources, held))]
    writes = [pltpu.make_async_copy(h, o, back.at[i]) for i, (h, o) in enumerate(zip(held, outs))]
    for read in reads:
        read.start()
    for read, write in zip(reads, writes):
        read.wait()
        write.start()
    for write in writes:
        write.wait()


def settle(arrays):
    hbm = pl.BlockSpec(memory_space=pl.ANY)
    dma = pltpu.SemaphoreType.DMA((len(arrays),))
    return pl.pallas_call(
        copy_kernel,
        out_shape=tuple(jax.ShapeDtypeStruct(a.shape, a.dtype) for a in arrays),
        in_specs=[hbm] * len(arrays),
        out_specs=(hbm,) * len(arrays),
        scratch_shapes=[pltpu.VMEM(a.shape, a.dtype) for a in arrays] + [dma, dma],
        name="settle",
    )(*arrays)


def local(queries, candidates, grades, query_weights):
    n_col, n_pb = lax.axis_size("col"), lax.axis_size("pb")
    rows, width = queries.shape
    half = candidates.shape[0]
    tall, cols = grades.shape
    scaling = 1.0 / math.sqrt(width)
    n_far = len(far_parts_of(half, n_pb))
    outs, chips = n_col // 4, n_col // 2
    chunk = min(LANES, half)
    n_x = half // chunk * (n_pb - 1)
    sub = rows // SUBS
    dma = pltpu.SemaphoreType.DMA
    vmem = pl.BlockSpec(memory_space=pltpu.VMEM)
    hbm = pl.BlockSpec(memory_space=pl.ANY)
    outputs = pl.pallas_call(
        functools.partial(kernel, n_col, n_pb, scaling, cols * n_col),
        out_shape=(
            jax.ShapeDtypeStruct((tall // LANES, LANES), F32),
            jax.ShapeDtypeStruct((rows, width), BF16),
            jax.ShapeDtypeStruct((half, width), BF16),
        ),
        in_specs=[hbm, hbm, hbm, vmem],
        out_specs=(vmem, vmem, vmem),
        scratch_shapes=[
            pltpu.VMEM((tall, width), BF16),
            pltpu.VMEM((cols, width), BF16),
            pltpu.VMEM((tall, cols), jnp.int32),
            pltpu.VMEM((cols, tall), jnp.int32),
            pltpu.VMEM((cols, tall), F32),
            pltpu.VMEM((cols, tall), BF16),
            pltpu.VMEM((chips, 1 + n_far, STATS, 2 * rows), F32),
            pltpu.VMEM((STATS, tall), F32),
            pltpu.VMEM((n_col, STATS, rows), F32),
            pltpu.VMEM((n_col, STATS, rows), F32),
            pltpu.VMEM((8, rows), F32),
            pltpu.VMEM((n_col, 8, rows), F32),
            pltpu.VMEM((chips, 2, rows, width), BF16),
            pltpu.VMEM((chips, rows, width), BF16),
            pltpu.VMEM((outs, rows, width), BF16),
            pltpu.VMEM((outs + 1, rows, width), BF16),
            pltpu.VMEM((outs, rows, width), BF16),
            pltpu.VMEM((sub, width), F32),
            pltpu.VMEM((n_x, chunk, width), BF16),
            pltpu.VMEM((half, width), F32),
            pltpu.VMEM((n_pb - 1, half, width), BF16),
            dma((2,)),
            dma((tall // (8 * LANES),)),
            dma((n_col, 4, SUBS)),
            dma((n_col, SUBS)),
            dma((n_far,)),
            dma((n_far,)),
            dma((n_col,)),
            dma((n_col,)),
            dma((n_col,)),
            dma((n_col,)),
            dma((chips,)),
            dma((chips,)),
            dma((outs, SUBS)),
            dma((outs, SUBS)),
            dma((outs, SUBS)),
            dma((outs + 1, SUBS)),
            dma((n_x,)),
            dma((n_x,)),
        ],
        compiler_params=pltpu.CompilerParams(
            collective_id=0, has_side_effects=True, vmem_limit_bytes=62 * 2**20
        ),
        name="listmle",
    )(queries, candidates, grades, query_weights.reshape(tall // LANES, LANES))
    losses, cand_grad, query_grad = settle((outputs[0], outputs[2], outputs[1]))
    return (losses.reshape(-1), query_grad, cand_grad)


def solution(mesh):
    in_specs = (P(("pb", "col"), None), P(("col", "pb"), None), P("pb", "col"), P("pb"))
    out_specs = (P("pb"), P(("pb", "col"), None), P(("col", "pb"), None))
    return jax.shard_map(local, mesh=mesh, in_specs=in_specs, out_specs=out_specs, check_vma=False)
```

```python
import functools
import math

import jax
import jax.numpy as jnp
from jax import lax
from jax.experimental import pallas as pl
from jax.experimental.pallas import tpu as pltpu
from jax.sharding import PartitionSpec as P

GRADES = 5
STATS = 16
COUNT_ROWS = (5, 6, 7, 14)
LOWEST = -1e30
LANES = 128
SUBS = 2
MESH = pl.DeviceIdType.MESH
F32 = jnp.float32
BF16 = jnp.bfloat16
LOG2E = math.log2(math.e)
LN2 = math.log(2.0)


class Place:
    def __init__(self, n_col, n_pb):
        assert n_col % 4 == 0
        self.n_col, self.n_pb = n_col, n_pb
        self.cores = self.mids = 2
        self.chips = n_col // 2
        self.outs = n_col // 4
        self.me = lax.axis_index("col")
        self.p = lax.axis_index("pb")
        self.core = lax.rem(self.me, 2)
        self.mid = lax.rem(self.me // 2, 2)
        self.out = self.me // 4

    def chip(self, out, dm):
        return out * 2 + lax.rem(self.mid + dm, 2)

    def block(self, out, dm, dc):
        return self.chip(out, dm) * 2 + lax.rem(self.core + dc, 2)

    def dev(self, col):
        return {"pb": self.p, "col": col}

    def visit(self, k):
        side = jnp.minimum(self.out, self.outs - 1 - self.out)
        near = (k + 1) // 2 * (2 * lax.rem(k, 2) - 1)
        far = (k - side) * jnp.where(2 * self.out < self.outs, 1, -1)
        return self.out + jnp.where(k <= 2 * side, near, far)

    def item(self, t):
        odd = (lax.rem(t, 2) == 1) & (t < self.chips - 1)
        first = t == 0
        v = jnp.where(odd, self.outs - 1 - (t + 1) // 2, self.outs - 1 - (t - 1) // 2)
        v = jnp.where(first, self.outs - 1, v)
        dm = jnp.where(odd | first, 1, 0)
        return self.visit(v), dm


def remote(src, dst, send, recv, device):
    return pltpu.make_async_remote_copy(
        src_ref=src, dst_ref=dst, send_sem=send, recv_sem=recv, device_id=device, device_id_type=MESH
    )


def span(block, size):
    return pl.ds(pl.multiple_of(block * size, size), size)


def statistics(s, g, put):
    tops = [jnp.max(jnp.where(g <= b, s, LOWEST), axis=0, keepdims=True) for b in range(GRADES - 1)]
    tops.append(jnp.max(s, axis=0, keepdims=True))
    picked = jnp.broadcast_to(tops[-1], s.shape)
    for b in range(GRADES - 2, -1, -1):
        picked = jnp.where(g <= b, tops[b], picked)
    e = jnp.exp2(s - picked)
    sums = [jnp.sum(jnp.where(g <= b, e, 0.0), axis=0, keepdims=True) for b in range(GRADES - 1)]
    sums.append(jnp.sum(e, axis=0, keepdims=True))
    for b in range(GRADES):
        put(b, tops[b])
        put(8 + b, sums[b] - sums[b - 1] if b else sums[b])
    put(8 + GRADES, jnp.sum(s, axis=0, keepdims=True))


def finish(got, n_col, cols, columns):
    G = GRADES
    rows = got.shape[2]
    graded = lax.broadcasted_iota(jnp.int32, (8, rows), 0) < G
    tops = got[0][:8]
    first = jnp.zeros_like(tops)
    for k in range(1, n_col):
        tops = jnp.maximum(tops, got[k][:8])
    second = first
    for k in range(n_col):
        block = got[k]
        first = first + block[:8]
        second = second + block[8:] * jnp.where(graded, jnp.exp2(block[:8] - tops), 1.0)
    top = [tops[b : b + 1] for b in range(G)]
    mass = [second[b : b + 1] for b in range(G)]
    total = second[G : G + 1]
    both = jnp.concatenate([first, second], axis=0)
    count = [both[r : r + 1] for r in COUNT_ROWS]
    count.append(float(cols * n_col) - (count[0] + count[1] + count[2] + count[3]))
    levels = []
    seen = jnp.zeros_like(total)
    summed = seen
    weighted = seen
    for b in range(G):
        seen = seen + count[b]
        summed = mass[b] if b == 0 else mass[b] + summed * jnp.exp2(top[b - 1] - top[b])
        present = seen > 0.0
        level = jnp.where(present, top[b] + jnp.log(jnp.where(present, summed, 1.0)) * LOG2E, top[b])
        levels.append(level)
        weighted = weighted + count[b] * level
    loss = (weighted - total) * (LN2 / columns)
    offsets = [None] * G
    factor = seen * 0.0
    for b in range(G - 1, -1, -1):
        own = count[b] * jnp.exp2(top[b] - levels[b])
        factor = own if b == G - 1 else own + factor * jnp.exp2(top[b] - top[b + 1])
        offsets[b] = jnp.log(jnp.maximum(factor, 1e-37)) * LOG2E - top[b]
    pad = jnp.zeros((8 - G - 1, loss.shape[1]), F32)
    return jnp.concatenate(offsets + [loss, pad], axis=0)


def far_parts_of(half, n_pb):
    sizes = [half // 2, half // 4, half // 4] if half % 512 == 0 else [half]
    return [(d, sum(sizes[:i]), n) for i, n in enumerate(sizes) for d in range(1, n_pb)]


def kernel(
    n_col, n_pb, scaling, columns,
    q_hbm, c_hbm, g_hbm, w_ref, loss_ref, q_out, c_out,
    q_all, c_all, g_raw, g_all, s_all, slopes, tables, counts, stats, got, mine, merged,
    q_part, core_got, y_got, z_got, z_part, acc, c_part, c_own, c_got,
    own_sem, g_sem, q_send, q_recv, c_send, c_recv, s_send, s_recv, m_send, m_recv,
    k_send, k_recv, y_send, y_recv, z_send, z_recv, x_send, x_recv,
):
    at = Place(n_col, n_pb)
    rows, width = q_hbm.shape
    half = c_hbm.shape[0]
    tall, cols = g_hbm.shape
    pair, quad = 2 * rows, 4 * rows
    sub = rows // SUBS
    outs, chips = at.outs, at.chips
    G = GRADES
    chunk = min(LANES, half)
    parts = far_parts_of(half, n_pb)
    n_far = len(parts)
    early = n_pb - 1

    own_q = pltpu.make_async_copy(q_hbm, q_all.at[span(at.me, rows)], own_sem.at[0])
    own_c = pltpu.make_async_copy(c_hbm, c_all.at[span(at.p, half)], own_sem.at[1])
    own_q.start()
    own_c.start()
    group = 8 * LANES
    g_copies = [
        pltpu.make_async_copy(g_hbm.at[pl.ds(h, group)], g_raw.at[pl.ds(h, group)], g_sem.at[h // group])
        for h in range(0, tall, group)
    ]
    for copy in g_copies:
        copy.start()
    barrier = pltpu.get_barrier_semaphore()
    for d in range(1, n_col):
        pl.semaphore_signal(
            barrier, inc=1, device_id=at.dev(lax.rem(at.me + d, n_col)), device_id_type=MESH
        )
    for d in range(1, n_pb):
        pl.semaphore_signal(
            barrier, inc=1, device_id={"pb": lax.rem(at.p + d, n_pb), "col": at.me}, device_id_type=MESH
        )
    pl.semaphore_wait(barrier, n_col + n_pb - 2)

    def q_span(block, s):
        return pl.ds(pl.multiple_of(block * rows + s * sub, sub), sub)

    def q_copy(block, s, t, col):
        ref = q_all.at[q_span(block, s)]
        return remote(ref, ref, q_send.at[block, t, s], q_recv.at[block, s], at.dev(col))

    def forward(k, dm, act, subs=range(SUBS)):
        out = at.visit(k)
        block = at.block(out, dm, 0)
        for s in subs:
            if act and not (isinstance(k, int) and k == 0 and dm == 0):
                q_copy(block, s, 0, at.me).wait_recv()

            def go(t, col):
                copy = q_copy(block, s, t, col)
                copy.start() if act else copy.wait_send()

            if dm == 0:
                @pl.when((out <= at.out) & (at.out < outs - 1))
                def _():
                    go(0, at.block(at.out + 1, 0, 0))

                @pl.when((out >= at.out) & (at.out > 0))
                def _():
                    go(1, at.block(at.out - 1, 0, 0))

                go(2, at.block(at.out, 1, 0))
            go(3, at.block(at.out, 0, 1))

    def partner(k, dm):
        block = at.block(at.visit(k), dm, 1)
        for s in range(SUBS):
            q_copy(block, s, 0, at.me).wait_recv()

    def c_copy(r):
        d, first, n = parts[r]
        ref = c_all.at[pl.ds(pl.multiple_of(at.p * half + first, n), n)]
        other = lax.rem(at.p + d, n_pb)
        return remote(ref, ref, c_send.at[r], c_recv.at[r], {"pb": other, "col": at.me})

    def c_first(r):
        d, first, n = parts[r]
        return lax.rem(at.p + n_pb - d, n_pb) * half + first

    def c_arrived(r):
        n = parts[r][2]
        ref = c_all.at[pl.ds(pl.multiple_of(c_first(r), n), n)]
        remote(ref, ref, c_send.at[r], c_recv.at[r], at.dev(at.me)).wait_recv()

    own_q.wait()
    forward(0, 0, True)
    counts[...] = jnp.zeros(counts.shape, F32)

    def clear(chip, carry):
        for h in range(n_far + 1):
            tables[chip, h] = jnp.zeros((STATS, pair), F32)
        return carry

    lax.fori_loop(0, chips, clear, 0)
    own_c.wait()
    for r in range(n_far):
        c_copy(r).start()

    assert cols % LANES == 0 and cols // 8 < 256 and tall % group == 0
    for h, copy in zip(range(0, tall, group), g_copies):
        copy.wait()

        def turn(k, codes, h=h):
            cc = span(k, LANES)
            word = g_raw[h : h + LANES, cc]
            for i in range(1, 8):
                word = word + jnp.left_shift(g_raw[h + i * LANES : h + (i + 1) * LANES, cc], 3 * i)
            word = word.T
            new = []
            for i in range(8):
                g = jnp.right_shift(word, 3 * i) & 7
                g_all[cc, h + i * LANES : h + (i + 1) * LANES] = g
                one = jnp.left_shift(1, g * 8)
                code = codes[i]
                for j in range(0, LANES, 8):
                    code = code + one[j : j + 8]
                new.append(code)
            return tuple(new)

        codes = lax.fori_loop(
            0, cols // LANES, turn, tuple(jnp.zeros((8, LANES), jnp.int32) for _ in range(8))
        )
        for i in range(8):
            for b in range(G - 1):
                field = (jnp.right_shift(codes[i], 8 * b) & 255).astype(F32)
                row = COUNT_ROWS[b]
                counts[row : row + 1, h + i * LANES : h + (i + 1) * LANES] = jnp.sum(field, axis=0, keepdims=True)

    def score(chip, wide, start, size, part):
        cc = pl.ds(pl.multiple_of(start, size), size)
        s = lax.dot_general(
            c_all[cc], q_all[pl.ds(pl.multiple_of(chip * pair, wide), wide)],
            (((1,), (1,)), ((), ())), preferred_element_type=F32,
        ) * (scaling * LOG2E)
        for x in range(0, wide, LANES):
            qq = pl.ds(pl.multiple_of(chip * pair + x, LANES), LANES)
            tile = s[:, x : x + LANES]
            s_all[cc, qq] = tile

            def put(i, row):
                tables[chip + x // pair, part, i : i + 1, x % pair : x % pair + LANES] = row

            statistics(tile, g_all[cc, qq], put)

    def near(k, dm):
        score(at.chip(at.visit(k), dm), pair, at.p * half, half, 0)

    def far(k, r, dm=None):
        chip, wide = (2 * at.visit(k), quad) if dm is None else (at.chip(at.visit(k), dm), pair)
        score(chip, wide, c_first(r), parts[r][2], r + 1)

    def each(last, task):
        lax.fori_loop(0, last, lambda j, c: (task(j), c)[1], 0)

    def stat_copy(block):
        return remote(stats.at[block], got.at[at.me], s_send.at[block], s_recv.at[at.me], at.dev(block))

    def join(ks):
        todo = [2 * at.visit(k) + m for k in ks for m in range(2)]
        for chip in todo:
            tabs = [tables[chip, h] for h in range(n_far + 1)]
            top = tabs[0][:8]
            for tab in tabs[1:]:
                top = jnp.maximum(top, tab[:8])
            mass = sum(tab[8:] * jnp.exp2(tab[:8] - top) for tab in tabs)
            count = counts[:, span(chip, pair)]
            for c in range(2):
                here = slice(c * rows, (c + 1) * rows)
                stats[chip * 2 + c, :8] = (top + count[:8])[:, here]
                stats[chip * 2 + c, 8:] = (mass + count[8:])[:, here]
        for chip in todo:
            for c in range(2):
                @pl.when(chip * 2 + c != at.me)
                def _():
                    stat_copy(chip * 2 + c).start()

    partner(0, 0)
    near(0, 0)
    if outs > 1:
        forward(1, 0, True, [0])

    def step(u, carry):
        forward(u, 0, True, range(1, SUBS))
        forward(u - 1, 1, True)
        partner(u - 1, 1)
        near(u - 1, 1)

        @pl.when(u + 1 < outs)
        def _():
            forward(u + 1, 0, True, [0])

        partner(u, 0)
        near(u, 0)

        @pl.when(u == 2)
        def _():
            for r in range(early):
                c_arrived(r)

        @pl.when(u >= 2)
        def _():
            for r in range(early):
                far(u - 2, r)

        return carry

    lax.fori_loop(1, outs, step, 0)
    if outs < 3:
        for r in range(early):
            c_arrived(r)
    for k in range(max(outs - 2, 0), outs - 1):
        for r in range(early):
            far(k, r)
    for r in range(n_far):
        if r >= early:
            c_arrived(r)
            each(outs - 1, lambda k, r=r: far(k, r))
        far(outs - 1, r, 0)

    forward(outs - 1, 1, True)

    join(range(outs - 1))
    partner(outs - 1, 1)
    near(outs - 1, 1)
    for r in range(n_far):
        far(outs - 1, r, 1)
    join([outs - 1])

    others = [lax.rem(at.me + d, n_col) for d in range(1, n_col)]
    got[at.me] = stats[at.me]
    for o in others:
        remote(stats.at[o], got.at[o], s_send.at[o], s_recv.at[o], at.dev(at.me)).wait_recv()
    mine[...] = finish(got, n_col, cols, columns)

    def merged_copy(o):
        return remote(mine, merged.at[at.me], m_send.at[o], m_recv.at[at.me], at.dev(o))

    for o in others:
        merged_copy(o).start()
    merged[at.me] = mine[...]
    for o in others:
        remote(mine, merged.at[o], m_send.at[o], m_recv.at[o], at.dev(at.me)).wait_recv()

    def slope(chip, start, size):
        qq = span(chip, pair)
        table = jnp.concatenate([merged[2 * chip], merged[2 * chip + 1]], axis=1)
        few = pair // LANES
        w = [w_ref[pl.ds(chip * few + x, 1), :] for x in range(few)]
        w = jnp.concatenate(w, axis=1)
        for x in range(0, pair, LANES):
            loss_ref[pl.ds(chip * (pair // LANES) + x // LANES, 1), :] = table[G : G + 1, x : x + LANES]

        def body(j, carry):
            cc = pl.ds(pl.multiple_of(start + j * chunk, chunk), chunk)
            g = g_all[cc, qq]
            off = jnp.broadcast_to(table[G - 1 : G], g.shape)
            for b in range(G - 2, -1, -1):
                off = jnp.where(g <= b, table[b : b + 1], off)
            slopes[cc, qq] = (w * jnp.exp2(s_all[cc, qq] + off) - w).astype(BF16)
            return carry

        if size == chunk:
            body(0, 0)
        else:
            lax.fori_loop(0, size // chunk, body, 0)

    def k_copy(chip):
        return remote(
            q_part.at[chip, lax.rem(at.core + 1, 2)], core_got.at[chip], k_send.at[chip], k_recv.at[chip],
            at.dev(at.block(at.out, 0, 1)),
        )

    def q_grad(t):
        out, dm = at.item(t)
        chip = at.chip(out, dm)
        part = lax.dot_general(
            slopes[:, span(chip, pair)], c_all[...], (((0,), (0,)), ((), ())), preferred_element_type=F32
        ) * scaling
        q_part[chip] = part.astype(BF16).reshape(2, rows, width)
        k_copy(chip).start()

    def sub_rows(s):
        return pl.ds(s * sub, sub)

    def y_copy(out, s):
        return remote(
            q_part.at[at.chip(out, 1), at.core, sub_rows(s)], y_got.at[out, sub_rows(s)],
            y_send.at[out, s], y_recv.at[out, s], at.dev(at.block(at.out, 1, 0)),
        )

    def cross(out):
        chip = at.chip(out, 1)
        k_copy(chip).wait_recv()
        for s in range(SUBS):
            rr = sub_rows(s)
            both = q_part[chip, at.core, rr].astype(F32) + core_got[chip, rr].astype(F32)
            q_part[chip, at.core, rr] = both.astype(BF16)
            y_copy(out, s).start()

    def z_copy(out, s):
        toward = jnp.where(out > at.out, at.out + 1, at.out - 1)
        slot = jnp.where((out < at.out) & (toward == out), outs, out)
        return remote(
            z_part.at[out, sub_rows(s)], z_got.at[slot, sub_rows(s)],
            z_send.at[out, s], z_recv.at[slot, s], at.dev(at.block(toward, 0, 0)),
        )

    def z_add(slot, s):
        ref = z_got.at[slot, sub_rows(s)]
        remote(ref, ref, z_send.at[0, s], z_recv.at[slot, s], at.dev(at.me)).wait_recv()
        acc[...] += z_got[slot, sub_rows(s)].astype(F32)

    def gather_row(out, s):
        chip = at.chip(out, 0)
        rr = sub_rows(s)
        ref = y_got.at[out, rr]
        remote(ref, ref, y_send.at[out, s], y_recv.at[out, s], at.dev(at.me)).wait_recv()
        acc[...] = (
            q_part[chip, at.core, rr].astype(F32)
            + core_got[chip, rr].astype(F32)
            + y_got[out, rr].astype(F32)
        )

    def chain(v):
        out = at.visit(v)
        k_copy(at.chip(out, 0)).wait_recv()
        behind = ((out > at.out) & (at.out > 0)) | ((out < at.out) & (at.out < outs - 1))
        for s in range(SUBS):
            gather_row(out, s)

            @pl.when(behind)
            def _():
                z_add(out, s)

            z_part[out, sub_rows(s)] = acc[...].astype(BF16)
            z_copy(out, s).start()

    per = half // chunk
    n_x = per * (n_pb - 1)

    def x_copy(r):
        d, j = 1 + r // per, lax.rem(r, per)
        other = lax.rem(at.p + d, n_pb)
        rr = pl.ds(pl.multiple_of(j * chunk, chunk), chunk)
        return remote(
            c_part.at[r], c_got.at[d - 1, rr], x_send.at[r], x_recv.at[r], {"pb": other, "col": at.me}
        )

    def c_grad(start):
        here = slopes[pl.ds(pl.multiple_of(start, chunk), chunk), :]
        return jnp.dot(here, q_all[...], preferred_element_type=F32) * scaling

    def c_far(r):
        other = lax.rem(at.p + 1 + r // per, n_pb)
        c_part[r] = c_grad(other * half + lax.rem(r, per) * chunk).astype(BF16)
        x_copy(r).start()

    def slope_first(i, carry):
        slope(i, lax.rem(at.p + 1, n_pb) * half, chunk)
        return carry

    def slope_step(i, carry):
        out, dm = at.item(i)
        slope(at.chip(out, dm), 0, cols)

        @pl.when(i == 0)
        def _():
            q_grad(0)

        @pl.when(i == 2)
        def _():
            cross(at.visit(outs - 1))

        return carry

    lax.fori_loop(0, chips, slope_first, 0)
    c_far(0)
    lax.fori_loop(0, chips, slope_step, 0)

    edge = (at.out == 0) | (at.out == outs - 1)

    def grad_step(j, carry):
        @pl.when((j > 0) & (j < n_x))
        def _():
            c_far(j)

        @pl.when(j + 1 < chips)
        def _():
            q_grad(j + 1)

        @pl.when((j >= 1) & (lax.rem(j, 2) == 1) & (j < chips - 1))
        def _():
            cross(at.item(j)[0])

        @pl.when((j == 2) & edge)
        def _():
            chain(outs - 1)

        return carry

    lax.fori_loop(0, max(n_x, chips - 1), grad_step, 0)

    def c_near(j, carry):
        c_own[pl.ds(pl.multiple_of(j * chunk, chunk), chunk)] = c_grad(at.p * half + j * chunk)
        return carry

    def chain_step(i, carry):
        @pl.when((i > 0) | jnp.logical_not(edge))
        def _():
            chain(outs - 1 - i)

        @pl.when((i == 0) & jnp.logical_not(edge) | (i == min(1, outs - 2)) & edge)
        def _():
            lax.fori_loop(0, per, c_near, 0)

        return carry

    lax.fori_loop(0, outs - 1, chain_step, 0)
    k_copy(at.chip(at.out, 0)).wait_recv()
    for s in range(SUBS):
        gather_row(at.out, s)

        @pl.when(at.out > 0)
        def _():
            z_add(at.out, s)

        @pl.when(at.out < outs - 1)
        def _():
            z_add(outs, s)

        q_out[sub_rows(s), :] = acc[...].astype(BF16)

    def c_finish(j, carry):
        rr = pl.ds(pl.multiple_of(j * chunk, chunk), chunk)
        total = c_own[rr]
        for d in range(1, n_pb):
            r = (d - 1) * per + j
            ref = c_got.at[d - 1, rr]
            remote(ref, ref, x_send.at[r], x_recv.at[r], at.dev(at.me)).wait_recv()
            total = total + c_got[d - 1, rr].astype(F32)
        c_out[rr] = total.astype(BF16)
        return carry

    lax.fori_loop(0, per, c_finish, 0)

    def drain(k, carry):
        for dm in range(2):
            forward(k, dm, False)
        out = at.visit(k)
        for dm in range(2):
            k_copy(at.chip(out, dm)).wait_send()
        for s in range(SUBS):
            y_copy(out, s).wait_send()

            @pl.when(k > 0)
            def _():
                z_copy(out, s).wait_send()

        return carry

    lax.fori_loop(0, outs, drain, 0)
    for r in range(n_far):
        c_copy(r).wait_send()
    for o in others:
        stat_copy(o).wait_send()
        merged_copy(o).wait_send()
    lax.fori_loop(0, n_x, lambda r, c: (x_copy(r).wait_send(), c)[1], 0)


def copy_kernel(*refs):
    n = (len(refs) - 2) // 3
    sources, outs, held = refs[:n], refs[n : 2 * n], refs[2 * n : 3 * n]
    into, back = refs[3 * n :]
    reads = [pltpu.make_async_copy(a, h, into.at[i]) for i, (a, h) in enumerate(zip(sources, held))]
    writes = [pltpu.make_async_copy(h, o, back.at[i]) for i, (h, o) in enumerate(zip(held, outs))]
    for read in reads:
        read.start()
    for read, write in zip(reads, writes):
        read.wait()
        write.start()
    for write in writes:
        write.wait()


def settle(arrays):
    hbm = pl.BlockSpec(memory_space=pl.ANY)
    dma = pltpu.SemaphoreType.DMA((len(arrays),))
    return pl.pallas_call(
        copy_kernel,
        out_shape=tuple(jax.ShapeDtypeStruct(a.shape, a.dtype) for a in arrays),
        in_specs=[hbm] * len(arrays),
        out_specs=(hbm,) * len(arrays),
        scratch_shapes=[pltpu.VMEM(a.shape, a.dtype) for a in arrays] + [dma, dma],
        name="settle",
    )(*arrays)


def local(queries, candidates, grades, query_weights):
    n_col, n_pb = lax.axis_size("col"), lax.axis_size("pb")
    rows, width = queries.shape
    half = candidates.shape[0]
    tall, cols = grades.shape
    scaling = 1.0 / math.sqrt(width)
    n_far = len(far_parts_of(half, n_pb))
    outs, chips = n_col // 4, n_col // 2
    chunk = min(LANES, half)
    n_x = half // chunk * (n_pb - 1)
    sub = rows // SUBS
    dma = pltpu.SemaphoreType.DMA
    vmem = pl.BlockSpec(memory_space=pltpu.VMEM)
    hbm = pl.BlockSpec(memory_space=pl.ANY)
    outputs = pl.pallas_call(
        functools.partial(kernel, n_col, n_pb, scaling, cols * n_col),
        out_shape=(
            jax.ShapeDtypeStruct((tall // LANES, LANES), F32),
            jax.ShapeDtypeStruct((rows, width), BF16),
            jax.ShapeDtypeStruct((half, width), BF16),
        ),
        in_specs=[hbm, hbm, hbm, vmem],
        out_specs=(vmem, vmem, vmem),
        scratch_shapes=[
            pltpu.VMEM((tall, width), BF16),
            pltpu.VMEM((cols, width), BF16),
            pltpu.VMEM((tall, cols), jnp.int32),
            pltpu.VMEM((cols, tall), jnp.int32),
            pltpu.VMEM((cols, tall), F32),
            pltpu.VMEM((cols, tall), BF16),
            pltpu.VMEM((chips, 1 + n_far, STATS, 2 * rows), F32),
            pltpu.VMEM((STATS, tall), F32),
            pltpu.VMEM((n_col, STATS, rows), F32),
            pltpu.VMEM((n_col, STATS, rows), F32),
            pltpu.VMEM((8, rows), F32),
            pltpu.VMEM((n_col, 8, rows), F32),
            pltpu.VMEM((chips, 2, rows, width), BF16),
            pltpu.VMEM((chips, rows, width), BF16),
            pltpu.VMEM((outs, rows, width), BF16),
            pltpu.VMEM((outs + 1, rows, width), BF16),
            pltpu.VMEM((outs, rows, width), BF16),
            pltpu.VMEM((sub, width), F32),
            pltpu.VMEM((n_x, chunk, width), BF16),
            pltpu.VMEM((half, width), F32),
            pltpu.VMEM((n_pb - 1, half, width), BF16),
            dma((2,)),
            dma((tall // (8 * LANES),)),
            dma((n_col, 4, SUBS)),
            dma((n_col, SUBS)),
            dma((n_far,)),
            dma((n_far,)),
            dma((n_col,)),
            dma((n_col,)),
            dma((n_col,)),
            dma((n_col,)),
            dma((chips,)),
            dma((chips,)),
            dma((outs, SUBS)),
            dma((outs, SUBS)),
            dma((outs, SUBS)),
            dma((outs + 1, SUBS)),
            dma((n_x,)),
            dma((n_x,)),
        ],
        compiler_params=pltpu.CompilerParams(
            collective_id=0, has_side_effects=True, vmem_limit_bytes=62 * 2**20
        ),
        name="listmle",
    )(queries, candidates, grades, query_weights.reshape(tall // LANES, LANES))
    losses, cand_grad, query_grad = settle((outputs[0], outputs[2], outputs[1]))
    return (losses.reshape(-1), query_grad, cand_grad)


def solution(mesh):
    in_specs = (P(("pb", "col"), None), P(("col", "pb"), None), P("pb", "col"), P("pb"))
    out_specs = (P("pb"), P(("pb", "col"), None), P(("col", "pb"), None))
    return jax.shard_map(local, mesh=mesh, in_specs=in_specs, out_specs=out_specs, check_vma=False)
```

```python
import functools
import math

import jax
import jax.numpy as jnp
from jax import lax
from jax.experimental import pallas as pl
from jax.experimental.pallas import tpu as pltpu
from jax.sharding import PartitionSpec as P

GRADES = 5
STATS = 16
COUNT_ROWS = (5, 6, 7, 14)
LOWEST = -1e30
LANES = 128
SUBS = 2
MESH = pl.DeviceIdType.MESH
F32 = jnp.float32
BF16 = jnp.bfloat16
LOG2E = math.log2(math.e)
LN2 = math.log(2.0)


class Place:
    def __init__(self, n_col, n_pb):
        assert n_col % 4 == 0
        self.n_col, self.n_pb = n_col, n_pb
        self.cores = self.mids = 2
        self.chips = n_col // 2
        self.outs = n_col // 4
        self.me = lax.axis_index("col")
        self.p = lax.axis_index("pb")
        self.core = lax.rem(self.me, 2)
        self.mid = lax.rem(self.me // 2, 2)
        self.out = self.me // 4

    def chip(self, out, dm):
        return out * 2 + lax.rem(self.mid + dm, 2)

    def block(self, out, dm, dc):
        return self.chip(out, dm) * 2 + lax.rem(self.core + dc, 2)

    def dev(self, col):
        return {"pb": self.p, "col": col}

    def visit(self, k):
        side = jnp.minimum(self.out, self.outs - 1 - self.out)
        near = (k + 1) // 2 * (2 * lax.rem(k, 2) - 1)
        far = (k - side) * jnp.where(2 * self.out < self.outs, 1, -1)
        return self.out + jnp.where(k <= 2 * side, near, far)

    def item(self, t):
        odd = (lax.rem(t, 2) == 1) & (t < self.chips - 1)
        first = t == 0
        v = jnp.where(odd, self.outs - 1 - (t + 1) // 2, self.outs - 1 - (t - 1) // 2)
        v = jnp.where(first, self.outs - 1, v)
        dm = jnp.where(odd | first, 1, 0)
        return self.visit(v), dm


def remote(src, dst, send, recv, device):
    return pltpu.make_async_remote_copy(
        src_ref=src, dst_ref=dst, send_sem=send, recv_sem=recv, device_id=device, device_id_type=MESH
    )


def span(block, size):
    return pl.ds(pl.multiple_of(block * size, size), size)


def statistics(s, g, put):
    tops = [jnp.max(jnp.where(g <= b, s, LOWEST), axis=0, keepdims=True) for b in range(GRADES - 1)]
    tops.append(jnp.max(s, axis=0, keepdims=True))
    picked = jnp.broadcast_to(tops[-1], s.shape)
    for b in range(GRADES - 2, -1, -1):
        picked = jnp.where(g <= b, tops[b], picked)
    e = jnp.exp2(s - picked)
    sums = [jnp.sum(jnp.where(g <= b, e, 0.0), axis=0, keepdims=True) for b in range(GRADES - 1)]
    sums.append(jnp.sum(e, axis=0, keepdims=True))
    for b in range(GRADES):
        put(b, tops[b])
        put(8 + b, sums[b] - sums[b - 1] if b else sums[b])
    put(8 + GRADES, jnp.sum(s, axis=0, keepdims=True))


def finish(got, n_col, cols, columns):
    G = GRADES
    rows = got.shape[2]
    graded = lax.broadcasted_iota(jnp.int32, (8, rows), 0) < G
    tops = got[0][:8]
    first = jnp.zeros_like(tops)
    for k in range(1, n_col):
        tops = jnp.maximum(tops, got[k][:8])
    second = first
    for k in range(n_col):
        block = got[k]
        first = first + block[:8]
        second = second + block[8:] * jnp.where(graded, jnp.exp2(block[:8] - tops), 1.0)
    top = [tops[b : b + 1] for b in range(G)]
    mass = [second[b : b + 1] for b in range(G)]
    total = second[G : G + 1]
    both = jnp.concatenate([first, second], axis=0)
    count = [both[r : r + 1] for r in COUNT_ROWS]
    count.append(float(cols * n_col) - (count[0] + count[1] + count[2] + count[3]))
    levels = []
    seen = jnp.zeros_like(total)
    summed = seen
    weighted = seen
    for b in range(G):
        seen = seen + count[b]
        summed = mass[b] if b == 0 else mass[b] + summed * jnp.exp2(top[b - 1] - top[b])
        present = seen > 0.0
        level = jnp.where(present, top[b] + jnp.log(jnp.where(present, summed, 1.0)) * LOG2E, top[b])
        levels.append(level)
        weighted = weighted + count[b] * level
    loss = (weighted - total) * (LN2 / columns)
    offsets = [None] * G
    factor = seen * 0.0
    for b in range(G - 1, -1, -1):
        own = count[b] * jnp.exp2(top[b] - levels[b])
        factor = own if b == G - 1 else own + factor * jnp.exp2(top[b] - top[b + 1])
        offsets[b] = jnp.log(jnp.maximum(factor, 1e-37)) * LOG2E - top[b]
    pad = jnp.zeros((8 - G - 1, loss.shape[1]), F32)
    return jnp.concatenate(offsets + [loss, pad], axis=0)


def far_parts_of(half, n_pb):
    sizes = [half // 2, half // 4, half // 4] if half % 512 == 0 else [half]
    return [(d, sum(sizes[:i]), n) for i, n in enumerate(sizes) for d in range(1, n_pb)]


def kernel(
    n_col, n_pb, scaling, columns,
    q_hbm, c_hbm, g_hbm, w_ref, loss_hbm, q_end, c_end, loss_ref, q_out, c_out,
    q_all, c_all, g_raw, g_all, s_all, slopes, tables, counts, stats, got, mine, merged,
    q_part, core_got, y_got, z_got, z_part, acc, c_part, c_own, c_got,
    out_sem, own_sem, g_sem, q_send, q_recv, c_send, c_recv, s_send, s_recv, m_send, m_recv,
    k_send, k_recv, y_send, y_recv, z_send, z_recv, x_send, x_recv,
):
    at = Place(n_col, n_pb)
    rows, width = q_hbm.shape
    half = c_hbm.shape[0]
    tall, cols = g_hbm.shape
    pair, quad = 2 * rows, 4 * rows
    sub = rows // SUBS
    outs, chips = at.outs, at.chips
    G = GRADES
    chunk = min(LANES, half)
    parts = far_parts_of(half, n_pb)
    n_far = len(parts)
    early = n_pb - 1

    own_q = pltpu.make_async_copy(q_hbm, q_all.at[span(at.me, rows)], own_sem.at[0])
    own_c = pltpu.make_async_copy(c_hbm, c_all.at[span(at.p, half)], own_sem.at[1])
    own_q.start()
    own_c.start()
    group = 8 * LANES
    g_copies = [
        pltpu.make_async_copy(g_hbm.at[pl.ds(h, group)], g_raw.at[pl.ds(h, group)], g_sem.at[h // group])
        for h in range(0, tall, group)
    ]
    for copy in g_copies:
        copy.start()
    barrier = pltpu.get_barrier_semaphore()
    for d in range(1, n_col):
        pl.semaphore_signal(
            barrier, inc=1, device_id=at.dev(lax.rem(at.me + d, n_col)), device_id_type=MESH
        )
    for d in range(1, n_pb):
        pl.semaphore_signal(
            barrier, inc=1, device_id={"pb": lax.rem(at.p + d, n_pb), "col": at.me}, device_id_type=MESH
        )
    pl.semaphore_wait(barrier, n_col + n_pb - 2)

    def q_span(block, s):
        return pl.ds(pl.multiple_of(block * rows + s * sub, sub), sub)

    def q_copy(block, s, t, col):
        ref = q_all.at[q_span(block, s)]
        return remote(ref, ref, q_send.at[block, t, s], q_recv.at[block, s], at.dev(col))

    def forward(k, dm, act, subs=range(SUBS)):
        out = at.visit(k)
        block = at.block(out, dm, 0)
        for s in subs:
            if act and not (isinstance(k, int) and k == 0 and dm == 0):
                q_copy(block, s, 0, at.me).wait_recv()

            def go(t, col):
                copy = q_copy(block, s, t, col)
                copy.start() if act else copy.wait_send()

            if dm == 0:
                @pl.when((out <= at.out) & (at.out < outs - 1))
                def _():
                    go(0, at.block(at.out + 1, 0, 0))

                @pl.when((out >= at.out) & (at.out > 0))
                def _():
                    go(1, at.block(at.out - 1, 0, 0))

                go(2, at.block(at.out, 1, 0))
            go(3, at.block(at.out, 0, 1))

    def partner(k, dm):
        block = at.block(at.visit(k), dm, 1)
        for s in range(SUBS):
            q_copy(block, s, 0, at.me).wait_recv()

    def c_copy(r):
        d, first, n = parts[r]
        ref = c_all.at[pl.ds(pl.multiple_of(at.p * half + first, n), n)]
        other = lax.rem(at.p + d, n_pb)
        return remote(ref, ref, c_send.at[r], c_recv.at[r], {"pb": other, "col": at.me})

    def c_first(r):
        d, first, n = parts[r]
        return lax.rem(at.p + n_pb - d, n_pb) * half + first

    def c_arrived(r):
        n = parts[r][2]
        ref = c_all.at[pl.ds(pl.multiple_of(c_first(r), n), n)]
        remote(ref, ref, c_send.at[r], c_recv.at[r], at.dev(at.me)).wait_recv()

    own_q.wait()
    forward(0, 0, True)
    counts[...] = jnp.zeros(counts.shape, F32)

    def clear(chip, carry):
        for h in range(n_far + 1):
            tables[chip, h] = jnp.zeros((STATS, pair), F32)
        return carry

    lax.fori_loop(0, chips, clear, 0)
    own_c.wait()
    for r in range(n_far):
        c_copy(r).start()

    assert cols % LANES == 0 and cols // 8 < 256 and tall % group == 0
    for h, copy in zip(range(0, tall, group), g_copies):
        copy.wait()

        def turn(k, codes, h=h):
            cc = span(k, LANES)
            word = g_raw[h : h + LANES, cc]
            for i in range(1, 8):
                word = word + jnp.left_shift(g_raw[h + i * LANES : h + (i + 1) * LANES, cc], 3 * i)
            word = word.T
            new = []
            for i in range(8):
                g = jnp.right_shift(word, 3 * i) & 7
                g_all[cc, h + i * LANES : h + (i + 1) * LANES] = g
                one = jnp.left_shift(1, g * 8)
                code = codes[i]
                for j in range(0, LANES, 8):
                    code = code + one[j : j + 8]
                new.append(code)
            return tuple(new)

        codes = lax.fori_loop(
            0, cols // LANES, turn, tuple(jnp.zeros((8, LANES), jnp.int32) for _ in range(8))
        )
        for i in range(8):
            for b in range(G - 1):
                field = (jnp.right_shift(codes[i], 8 * b) & 255).astype(F32)
                row = COUNT_ROWS[b]
                counts[row : row + 1, h + i * LANES : h + (i + 1) * LANES] = jnp.sum(field, axis=0, keepdims=True)

    def score(chip, wide, start, size, part):
        cc = pl.ds(pl.multiple_of(start, size), size)
        s = lax.dot_general(
            c_all[cc], q_all[pl.ds(pl.multiple_of(chip * pair, wide), wide)],
            (((1,), (1,)), ((), ())), preferred_element_type=F32,
        ) * (scaling * LOG2E)
        for x in range(0, wide, LANES):
            qq = pl.ds(pl.multiple_of(chip * pair + x, LANES), LANES)
            tile = s[:, x : x + LANES]
            s_all[cc, qq] = tile

            def put(i, row):
                tables[chip + x // pair, part, i : i + 1, x % pair : x % pair + LANES] = row

            statistics(tile, g_all[cc, qq], put)

    def near(k, dm):
        score(at.chip(at.visit(k), dm), pair, at.p * half, half, 0)

    def far(k, r):
        score(2 * at.visit(k), quad, c_first(r), parts[r][2], r + 1)

    def each(last, task):
        lax.fori_loop(0, last, lambda j, c: (task(j), c)[1], 0)

    def stat_copy(block):
        return remote(stats.at[block], got.at[at.me], s_send.at[block], s_recv.at[at.me], at.dev(block))

    def join(ks):
        todo = [2 * at.visit(k) + m for k in ks for m in range(2)]
        for chip in todo:
            tabs = [tables[chip, h] for h in range(n_far + 1)]
            top = tabs[0][:8]
            for tab in tabs[1:]:
                top = jnp.maximum(top, tab[:8])
            mass = sum(tab[8:] * jnp.exp2(tab[:8] - top) for tab in tabs)
            count = counts[:, span(chip, pair)]
            for c in range(2):
                here = slice(c * rows, (c + 1) * rows)
                stats[chip * 2 + c, :8] = (top + count[:8])[:, here]
                stats[chip * 2 + c, 8:] = (mass + count[8:])[:, here]
        for chip in todo:
            for c in range(2):
                @pl.when(chip * 2 + c != at.me)
                def _():
                    stat_copy(chip * 2 + c).start()

    partner(0, 0)
    near(0, 0)
    if outs > 1:
        forward(1, 0, True, [0])

    def step(u, carry):
        forward(u, 0, True, range(1, SUBS))
        forward(u - 1, 1, True)
        partner(u - 1, 1)
        near(u - 1, 1)

        @pl.when(u + 1 < outs)
        def _():
            forward(u + 1, 0, True, [0])

        partner(u, 0)
        near(u, 0)

        @pl.when(u == 2)
        def _():
            for r in range(early):
                c_arrived(r)

        @pl.when(u >= 2)
        def _():
            for r in range(early):
                far(u - 2, r)

        return carry

    lax.fori_loop(1, outs, step, 0)
    if outs < 3:
        for r in range(early):
            c_arrived(r)
    for k in range(max(outs - 2, 0), outs - 1):
        for r in range(early):
            far(k, r)
    for r in range(early, n_far):
        if r == n_far - early:
            forward(outs - 1, 1, True)
        c_arrived(r)
        each(outs - 1, lambda k, r=r: far(k, r))
    if n_far == early:
        forward(outs - 1, 1, True)
    join(range(outs - 1))
    partner(outs - 1, 1)
    near(outs - 1, 1)
    for r in range(n_far):
        far(outs - 1, r)
    join([outs - 1])

    others = [lax.rem(at.me + d, n_col) for d in range(1, n_col)]
    got[at.me] = stats[at.me]
    for o in others:
        remote(stats.at[o], got.at[o], s_send.at[o], s_recv.at[o], at.dev(at.me)).wait_recv()
    mine[...] = finish(got, n_col, cols, columns)

    def merged_copy(o):
        return remote(mine, merged.at[at.me], m_send.at[o], m_recv.at[at.me], at.dev(o))

    for o in others:
        merged_copy(o).start()
    merged[at.me] = mine[...]
    for o in others:
        remote(mine, merged.at[o], m_send.at[o], m_recv.at[o], at.dev(at.me)).wait_recv()

    def slope(chip, start, size):
        qq = span(chip, pair)
        table = jnp.concatenate([merged[2 * chip], merged[2 * chip + 1]], axis=1)
        few = pair // LANES
        w = [w_ref[pl.ds(chip * few + x, 1), :] for x in range(few)]
        w = jnp.concatenate(w, axis=1)
        for x in range(0, pair, LANES):
            loss_ref[pl.ds(chip * (pair // LANES) + x // LANES, 1), :] = table[G : G + 1, x : x + LANES]

        def body(j, carry):
            cc = pl.ds(pl.multiple_of(start + j * chunk, chunk), chunk)
            g = g_all[cc, qq]
            off = jnp.broadcast_to(table[G - 1 : G], g.shape)
            for b in range(G - 2, -1, -1):
                off = jnp.where(g <= b, table[b : b + 1], off)
            slopes[cc, qq] = (w * jnp.exp2(s_all[cc, qq] + off) - w).astype(BF16)
            return carry

        if size == chunk:
            body(0, 0)
        else:
            lax.fori_loop(0, size // chunk, body, 0)

    def k_copy(chip):
        return remote(
            q_part.at[chip, lax.rem(at.core + 1, 2)], core_got.at[chip], k_send.at[chip], k_recv.at[chip],
            at.dev(at.block(at.out, 0, 1)),
        )

    def q_grad(t):
        out, dm = at.item(t)
        chip = at.chip(out, dm)
        part = lax.dot_general(
            slopes[:, span(chip, pair)], c_all[...], (((0,), (0,)), ((), ())), preferred_element_type=F32
        ) * scaling
        q_part[chip] = part.astype(BF16).reshape(2, rows, width)
        k_copy(chip).start()

    def sub_rows(s):
        return pl.ds(s * sub, sub)

    def y_copy(out, s):
        return remote(
            q_part.at[at.chip(out, 1), at.core, sub_rows(s)], y_got.at[out, sub_rows(s)],
            y_send.at[out, s], y_recv.at[out, s], at.dev(at.block(at.out, 1, 0)),
        )

    def cross(out):
        chip = at.chip(out, 1)
        k_copy(chip).wait_recv()
        for s in range(SUBS):
            rr = sub_rows(s)
            both = q_part[chip, at.core, rr].astype(F32) + core_got[chip, rr].astype(F32)
            q_part[chip, at.core, rr] = both.astype(BF16)
            y_copy(out, s).start()

    def z_copy(out, s):
        toward = jnp.where(out > at.out, at.out + 1, at.out - 1)
        slot = jnp.where((out < at.out) & (toward == out), outs, out)
        return remote(
            z_part.at[out, sub_rows(s)], z_got.at[slot, sub_rows(s)],
            z_send.at[out, s], z_recv.at[slot, s], at.dev(at.block(toward, 0, 0)),
        )

    def z_add(slot, s):
        ref = z_got.at[slot, sub_rows(s)]
        remote(ref, ref, z_send.at[0, s], z_recv.at[slot, s], at.dev(at.me)).wait_recv()
        acc[...] += z_got[slot, sub_rows(s)].astype(F32)

    def gather_row(out, s):
        chip = at.chip(out, 0)
        rr = sub_rows(s)
        ref = y_got.at[out, rr]
        remote(ref, ref, y_send.at[out, s], y_recv.at[out, s], at.dev(at.me)).wait_recv()
        acc[...] = (
            q_part[chip, at.core, rr].astype(F32)
            + core_got[chip, rr].astype(F32)
            + y_got[out, rr].astype(F32)
        )

    def chain(v):
        out = at.visit(v)
        k_copy(at.chip(out, 0)).wait_recv()
        behind = ((out > at.out) & (at.out > 0)) | ((out < at.out) & (at.out < outs - 1))
        for s in range(SUBS):
            gather_row(out, s)

            @pl.when(behind)
            def _():
                z_add(out, s)

            z_part[out, sub_rows(s)] = acc[...].astype(BF16)
            z_copy(out, s).start()

    per = half // chunk
    n_x = per * (n_pb - 1)

    def x_copy(r):
        d, j = 1 + r // per, lax.rem(r, per)
        other = lax.rem(at.p + d, n_pb)
        rr = pl.ds(pl.multiple_of(j * chunk, chunk), chunk)
        return remote(
            c_part.at[r], c_got.at[d - 1, rr], x_send.at[r], x_recv.at[r], {"pb": other, "col": at.me}
        )

    def c_grad(start):
        here = slopes[pl.ds(pl.multiple_of(start, chunk), chunk), :]
        return jnp.dot(here, q_all[...], preferred_element_type=F32) * scaling

    def c_far(r):
        other = lax.rem(at.p + 1 + r // per, n_pb)
        c_part[r] = c_grad(other * half + lax.rem(r, per) * chunk).astype(BF16)
        x_copy(r).start()

    def slope_first(i, carry):
        slope(i, lax.rem(at.p + 1, n_pb) * half, chunk)
        return carry

    def slope_step(i, carry):
        out, dm = at.item(i)
        slope(at.chip(out, dm), 0, cols)

        @pl.when(i == 0)
        def _():
            q_grad(0)

        @pl.when(i == 2)
        def _():
            cross(at.visit(outs - 1))

        return carry

    lax.fori_loop(0, chips, slope_first, 0)
    c_far(0)
    lax.fori_loop(0, chips, slope_step, 0)

    edge = (at.out == 0) | (at.out == outs - 1)

    def grad_step(j, carry):
        @pl.when((j > 0) & (j < n_x))
        def _():
            c_far(j)

        @pl.when(j + 1 < chips)
        def _():
            q_grad(j + 1)

        @pl.when((j >= 1) & (lax.rem(j, 2) == 1) & (j < chips - 1))
        def _():
            cross(at.item(j)[0])

        @pl.when((j == 2) & edge)
        def _():
            chain(outs - 1)

        return carry

    lax.fori_loop(0, max(n_x, chips - 1), grad_step, 0)

    def c_near(j, carry):
        c_own[pl.ds(pl.multiple_of(j * chunk, chunk), chunk)] = c_grad(at.p * half + j * chunk)
        return carry

    def chain_step(i, carry):
        @pl.when((i > 0) | jnp.logical_not(edge))
        def _():
            chain(outs - 1 - i)

        @pl.when((i == 0) & jnp.logical_not(edge) | (i == min(1, outs - 2)) & edge)
        def _():
            lax.fori_loop(0, per, c_near, 0)

        return carry

    lax.fori_loop(0, outs - 1, chain_step, 0)
    k_copy(at.chip(at.out, 0)).wait_recv()
    for s in range(SUBS):
        gather_row(at.out, s)

        @pl.when(at.out > 0)
        def _():
            z_add(at.out, s)

        @pl.when(at.out < outs - 1)
        def _():
            z_add(outs, s)

        q_out[sub_rows(s), :] = acc[...].astype(BF16)

    loss_copy = pltpu.make_async_copy(loss_ref, loss_hbm, out_sem.at[0])
    q_end_copy = pltpu.make_async_copy(q_out, q_end, out_sem.at[1])
    loss_copy.start()
    q_end_copy.start()

    def c_end_copy(j):
        rr = pl.ds(pl.multiple_of(j * chunk, chunk), chunk)
        return pltpu.make_async_copy(c_out.at[rr], c_end.at[rr], out_sem.at[2 + j])

    def c_finish(j, carry):
        rr = pl.ds(pl.multiple_of(j * chunk, chunk), chunk)
        total = c_own[rr]
        for d in range(1, n_pb):
            r = (d - 1) * per + j
            ref = c_got.at[d - 1, rr]
            remote(ref, ref, x_send.at[r], x_recv.at[r], at.dev(at.me)).wait_recv()
            total = total + c_got[d - 1, rr].astype(F32)
        c_out[rr] = total.astype(BF16)
        c_end_copy(j).start()
        return carry

    lax.fori_loop(0, per, c_finish, 0)

    def drain(k, carry):
        for dm in range(2):
            forward(k, dm, False)
        out = at.visit(k)
        for dm in range(2):
            k_copy(at.chip(out, dm)).wait_send()
        for s in range(SUBS):
            y_copy(out, s).wait_send()

            @pl.when(k > 0)
            def _():
                z_copy(out, s).wait_send()

        return carry

    lax.fori_loop(0, outs, drain, 0)
    for r in range(n_far):
        c_copy(r).wait_send()
    for o in others:
        stat_copy(o).wait_send()
        merged_copy(o).wait_send()
    lax.fori_loop(0, n_x, lambda r, c: (x_copy(r).wait_send(), c)[1], 0)
    loss_copy.wait()
    q_end_copy.wait()
    lax.fori_loop(0, per, lambda j, c: (c_end_copy(j).wait(), c)[1], 0)


def copy_kernel(*refs):
    n = (len(refs) - 2) // 3
    sources, outs, held = refs[:n], refs[n : 2 * n], refs[2 * n : 3 * n]
    into, back = refs[3 * n :]
    reads = [pltpu.make_async_copy(a, h, into.at[i]) for i, (a, h) in enumerate(zip(sources, held))]
    writes = [pltpu.make_async_copy(h, o, back.at[i]) for i, (h, o) in enumerate(zip(held, outs))]
    for read in reads:
        read.start()
    for read, write in zip(reads, writes):
        read.wait()
        write.start()
    for write in writes:
        write.wait()


def settle(arrays):
    hbm = pl.BlockSpec(memory_space=pl.ANY)
    dma = pltpu.SemaphoreType.DMA((len(arrays),))
    return pl.pallas_call(
        copy_kernel,
        out_shape=tuple(jax.ShapeDtypeStruct(a.shape, a.dtype) for a in arrays),
        in_specs=[hbm] * len(arrays),
        out_specs=(hbm,) * len(arrays),
        scratch_shapes=[pltpu.VMEM(a.shape, a.dtype) for a in arrays] + [dma, dma],
        name="settle",
    )(*arrays)


def local(queries, candidates, grades, query_weights):
    n_col, n_pb = lax.axis_size("col"), lax.axis_size("pb")
    rows, width = queries.shape
    half = candidates.shape[0]
    tall, cols = grades.shape
    scaling = 1.0 / math.sqrt(width)
    n_far = len(far_parts_of(half, n_pb))
    outs, chips = n_col // 4, n_col // 2
    chunk = min(LANES, half)
    n_x = half // chunk * (n_pb - 1)
    sub = rows // SUBS
    dma = pltpu.SemaphoreType.DMA
    vmem = pl.BlockSpec(memory_space=pltpu.VMEM)
    hbm = pl.BlockSpec(memory_space=pl.ANY)
    outputs = pl.pallas_call(
        functools.partial(kernel, n_col, n_pb, scaling, cols * n_col),
        out_shape=(
            jax.ShapeDtypeStruct((tall // LANES, LANES), F32),
            jax.ShapeDtypeStruct((rows, width), BF16),
            jax.ShapeDtypeStruct((half, width), BF16),
        ),
        in_specs=[hbm, hbm, hbm, vmem],
        out_specs=(hbm, hbm, hbm),
        scratch_shapes=[
            pltpu.VMEM((tall // LANES, LANES), F32),
            pltpu.VMEM((rows, width), BF16),
            pltpu.VMEM((half, width), BF16),
            pltpu.VMEM((tall, width), BF16),
            pltpu.VMEM((cols, width), BF16),
            pltpu.VMEM((tall, cols), jnp.int32),
            pltpu.VMEM((cols, tall), jnp.int32),
            pltpu.VMEM((cols, tall), F32),
            pltpu.VMEM((cols, tall), BF16),
            pltpu.VMEM((chips, 1 + n_far, STATS, 2 * rows), F32),
            pltpu.VMEM((STATS, tall), F32),
            pltpu.VMEM((n_col, STATS, rows), F32),
            pltpu.VMEM((n_col, STATS, rows), F32),
            pltpu.VMEM((8, rows), F32),
            pltpu.VMEM((n_col, 8, rows), F32),
            pltpu.VMEM((chips, 2, rows, width), BF16),
            pltpu.VMEM((chips, rows, width), BF16),
            pltpu.VMEM((outs, rows, width), BF16),
            pltpu.VMEM((outs + 1, rows, width), BF16),
            pltpu.VMEM((outs, rows, width), BF16),
            pltpu.VMEM((sub, width), F32),
            pltpu.VMEM((n_x, chunk, width), BF16),
            pltpu.VMEM((half, width), F32),
            pltpu.VMEM((n_pb - 1, half, width), BF16),
            dma((2 + half // chunk,)),
            dma((2,)),
            dma((tall // (8 * LANES),)),
            dma((n_col, 4, SUBS)),
            dma((n_col, SUBS)),
            dma((n_far,)),
            dma((n_far,)),
            dma((n_col,)),
            dma((n_col,)),
            dma((n_col,)),
            dma((n_col,)),
            dma((chips,)),
            dma((chips,)),
            dma((outs, SUBS)),
            dma((outs, SUBS)),
            dma((outs, SUBS)),
            dma((outs + 1, SUBS)),
            dma((n_x,)),
            dma((n_x,)),
        ],
        compiler_params=pltpu.CompilerParams(
            collective_id=0, has_side_effects=True, vmem_limit_bytes=62 * 2**20
        ),
        name="listmle",
    )(queries, candidates, grades, query_weights.reshape(tall // LANES, LANES))
    losses, cand_grad, query_grad = settle((outputs[0], outputs[2], outputs[1]))
    return (losses.reshape(-1), query_grad, cand_grad)


def solution(mesh):
    in_specs = (P(("pb", "col"), None), P(("col", "pb"), None), P("pb", "col"), P("pb"))
    out_specs = (P("pb"), P(("pb", "col"), None), P(("col", "pb"), None))
    return jax.shard_map(local, mesh=mesh, in_specs=in_specs, out_specs=out_specs, check_vma=False)
```

```python
import functools
import math

import jax
import jax.numpy as jnp
from jax import lax
from jax.experimental import pallas as pl
from jax.experimental.pallas import tpu as pltpu
from jax.sharding import PartitionSpec as P

GRADES = 5
STATS = 16
COUNT_ROWS = (5, 6, 7, 14)
LOWEST = -1e30
LANES = 128
SUBS = 2
MESH = pl.DeviceIdType.MESH
F32 = jnp.float32
BF16 = jnp.bfloat16
LOG2E = math.log2(math.e)
LN2 = math.log(2.0)


class Place:
    def __init__(self, n_col, n_pb):
        assert n_col % 4 == 0
        self.n_col, self.n_pb = n_col, n_pb
        self.cores = self.mids = 2
        self.chips = n_col // 2
        self.outs = n_col // 4
        self.me = lax.axis_index("col")
        self.p = lax.axis_index("pb")
        self.core = lax.rem(self.me, 2)
        self.mid = lax.rem(self.me // 2, 2)
        self.out = self.me // 4

    def chip(self, out, dm):
        return out * 2 + lax.rem(self.mid + dm, 2)

    def block(self, out, dm, dc):
        return self.chip(out, dm) * 2 + lax.rem(self.core + dc, 2)

    def dev(self, col):
        return {"pb": self.p, "col": col}

    def visit(self, k):
        side = jnp.minimum(self.out, self.outs - 1 - self.out)
        near = (k + 1) // 2 * (2 * lax.rem(k, 2) - 1)
        far = (k - side) * jnp.where(2 * self.out < self.outs, 1, -1)
        return self.out + jnp.where(k <= 2 * side, near, far)

    def item(self, t):
        odd = (lax.rem(t, 2) == 1) & (t < self.chips - 1)
        first = t == 0
        v = jnp.where(odd, self.outs - 1 - (t + 1) // 2, self.outs - 1 - (t - 1) // 2)
        v = jnp.where(first, self.outs - 1, v)
        dm = jnp.where(odd | first, 1, 0)
        return self.visit(v), dm


def remote(src, dst, send, recv, device):
    return pltpu.make_async_remote_copy(
        src_ref=src, dst_ref=dst, send_sem=send, recv_sem=recv, device_id=device, device_id_type=MESH
    )


def span(block, size):
    return pl.ds(pl.multiple_of(block * size, size), size)


def statistics(s, g, put):
    tops = [jnp.max(jnp.where(g <= b, s, LOWEST), axis=0, keepdims=True) for b in range(GRADES - 1)]
    tops.append(jnp.max(s, axis=0, keepdims=True))
    e = jnp.exp2(s - pick(jnp.concatenate(tops + [tops[-1]] * (8 - GRADES), axis=0), g))
    sums = [jnp.sum(jnp.where(g <= b, e, 0.0), axis=0, keepdims=True) for b in range(GRADES - 1)]
    sums.append(jnp.sum(e, axis=0, keepdims=True))
    for b in range(GRADES):
        put(b, tops[b])
        put(8 + b, sums[b] - sums[b - 1] if b else sums[b])
    put(8 + GRADES, jnp.sum(s, axis=0, keepdims=True))


def pick(table, g):
    tiles = [
        [jnp.take_along_axis(table[:, x : x + LANES], g[r : r + 8, x : x + LANES], axis=0) for x in range(0, g.shape[1], LANES)]
        for r in range(0, g.shape[0], 8)
    ]
    return jnp.concatenate([jnp.concatenate(row, axis=1) for row in tiles], axis=0)


def finish(got, n_col, cols, columns):
    G = GRADES
    rows = got.shape[2]
    graded = lax.broadcasted_iota(jnp.int32, (8, rows), 0) < G
    tops = got[0][:8]
    first = jnp.zeros_like(tops)
    for k in range(1, n_col):
        tops = jnp.maximum(tops, got[k][:8])
    second = first
    for k in range(n_col):
        block = got[k]
        first = first + block[:8]
        second = second + block[8:] * jnp.where(graded, jnp.exp2(block[:8] - tops), 1.0)
    top = [tops[b : b + 1] for b in range(G)]
    mass = [second[b : b + 1] for b in range(G)]
    total = second[G : G + 1]
    both = jnp.concatenate([first, second], axis=0)
    count = [both[r : r + 1] for r in COUNT_ROWS]
    count.append(float(cols * n_col) - (count[0] + count[1] + count[2] + count[3]))
    levels = []
    seen = jnp.zeros_like(total)
    summed = seen
    weighted = seen
    for b in range(G):
        seen = seen + count[b]
        summed = mass[b] if b == 0 else mass[b] + summed * jnp.exp2(top[b - 1] - top[b])
        present = seen > 0.0
        level = jnp.where(present, top[b] + jnp.log(jnp.where(present, summed, 1.0)) * LOG2E, top[b])
        levels.append(level)
        weighted = weighted + count[b] * level
    loss = (weighted - total) * (LN2 / columns)
    offsets = [None] * G
    factor = seen * 0.0
    for b in range(G - 1, -1, -1):
        own = count[b] * jnp.exp2(top[b] - levels[b])
        factor = own if b == G - 1 else own + factor * jnp.exp2(top[b] - top[b + 1])
        offsets[b] = jnp.log(jnp.maximum(factor, 1e-37)) * LOG2E - top[b]
    pad = jnp.zeros((8 - G - 1, loss.shape[1]), F32)
    return jnp.concatenate(offsets + [loss, pad], axis=0)


def far_parts_of(half, n_pb):
    sizes = [half // 2, half // 4, half // 4] if half % 512 == 0 else [half]
    return [(d, sum(sizes[:i]), n) for i, n in enumerate(sizes) for d in range(1, n_pb)]


def kernel(
    n_col, n_pb, scaling, columns,
    q_hbm, c_hbm, g_hbm, w_ref, loss_hbm, q_end, c_end, loss_ref, q_out, c_out,
    q_all, c_all, g_raw, g_all, s_all, slopes, tables, counts, stats, got, mine, merged,
    q_part, core_got, y_got, z_got, z_part, acc, c_part, c_own, c_got,
    out_sem, own_sem, g_sem, q_send, q_recv, c_send, c_recv, s_send, s_recv, m_send, m_recv,
    k_send, k_recv, y_send, y_recv, z_send, z_recv, x_send, x_recv,
):
    at = Place(n_col, n_pb)
    rows, width = q_hbm.shape
    half = c_hbm.shape[0]
    tall, cols = g_hbm.shape
    pair, quad = 2 * rows, 4 * rows
    sub = rows // SUBS
    outs, chips = at.outs, at.chips
    G = GRADES
    chunk = min(LANES, half)
    parts = far_parts_of(half, n_pb)
    n_far = len(parts)
    early = n_pb - 1

    own_q = pltpu.make_async_copy(q_hbm, q_all.at[span(at.me, rows)], own_sem.at[0])
    own_c = pltpu.make_async_copy(c_hbm, c_all.at[span(at.p, half)], own_sem.at[1])
    own_q.start()
    own_c.start()
    group = 8 * LANES
    g_copies = [
        pltpu.make_async_copy(g_hbm.at[pl.ds(h, group)], g_raw.at[pl.ds(h, group)], g_sem.at[h // group])
        for h in range(0, tall, group)
    ]
    for copy in g_copies:
        copy.start()
    barrier = pltpu.get_barrier_semaphore()
    for d in range(1, n_col):
        pl.semaphore_signal(
            barrier, inc=1, device_id=at.dev(lax.rem(at.me + d, n_col)), device_id_type=MESH
        )
    for d in range(1, n_pb):
        pl.semaphore_signal(
            barrier, inc=1, device_id={"pb": lax.rem(at.p + d, n_pb), "col": at.me}, device_id_type=MESH
        )
    pl.semaphore_wait(barrier, n_col + n_pb - 2)

    def q_span(block, s):
        return pl.ds(pl.multiple_of(block * rows + s * sub, sub), sub)

    def q_copy(block, s, t, col):
        ref = q_all.at[q_span(block, s)]
        return remote(ref, ref, q_send.at[block, t, s], q_recv.at[block, s], at.dev(col))

    def forward(k, dm, act, subs=range(SUBS)):
        out = at.visit(k)
        block = at.block(out, dm, 0)
        for s in subs:
            if act and not (isinstance(k, int) and k == 0 and dm == 0):
                q_copy(block, s, 0, at.me).wait_recv()

            def go(t, col):
                copy = q_copy(block, s, t, col)
                copy.start() if act else copy.wait_send()

            if dm == 0:
                @pl.when((out <= at.out) & (at.out < outs - 1))
                def _():
                    go(0, at.block(at.out + 1, 0, 0))

                @pl.when((out >= at.out) & (at.out > 0))
                def _():
                    go(1, at.block(at.out - 1, 0, 0))

                go(2, at.block(at.out, 1, 0))
            go(3, at.block(at.out, 0, 1))

    def partner(k, dm):
        block = at.block(at.visit(k), dm, 1)
        for s in range(SUBS):
            q_copy(block, s, 0, at.me).wait_recv()

    def c_copy(r):
        d, first, n = parts[r]
        ref = c_all.at[pl.ds(pl.multiple_of(at.p * half + first, n), n)]
        other = lax.rem(at.p + d, n_pb)
        return remote(ref, ref, c_send.at[r], c_recv.at[r], {"pb": other, "col": at.me})

    def c_first(r):
        d, first, n = parts[r]
        return lax.rem(at.p + n_pb - d, n_pb) * half + first

    def c_arrived(r):
        n = parts[r][2]
        ref = c_all.at[pl.ds(pl.multiple_of(c_first(r), n), n)]
        remote(ref, ref, c_send.at[r], c_recv.at[r], at.dev(at.me)).wait_recv()

    own_q.wait()
    forward(0, 0, True)
    counts[...] = jnp.zeros(counts.shape, F32)

    def clear(chip, carry):
        for h in range(n_far + 1):
            tables[chip, h] = jnp.zeros((STATS, pair), F32)
        return carry

    lax.fori_loop(0, chips, clear, 0)
    own_c.wait()
    for r in range(n_far):
        c_copy(r).start()

    assert cols % LANES == 0 and cols // 8 < 256 and tall % group == 0
    for h, copy in zip(range(0, tall, group), g_copies):
        copy.wait()

        def turn(k, codes, h=h):
            cc = span(k, LANES)
            word = g_raw[h : h + LANES, cc]
            for i in range(1, 8):
                word = word + jnp.left_shift(g_raw[h + i * LANES : h + (i + 1) * LANES, cc], 3 * i)
            word = word.T
            new = []
            for i in range(8):
                g = jnp.right_shift(word, 3 * i) & 7
                g_all[cc, h + i * LANES : h + (i + 1) * LANES] = g
                one = jnp.left_shift(1, g * 8)
                code = codes[i]
                for j in range(0, LANES, 8):
                    code = code + one[j : j + 8]
                new.append(code)
            return tuple(new)

        codes = lax.fori_loop(
            0, cols // LANES, turn, tuple(jnp.zeros((8, LANES), jnp.int32) for _ in range(8))
        )
        for i in range(8):
            for b in range(G - 1):
                field = (jnp.right_shift(codes[i], 8 * b) & 255).astype(F32)
                row = COUNT_ROWS[b]
                counts[row : row + 1, h + i * LANES : h + (i + 1) * LANES] = jnp.sum(field, axis=0, keepdims=True)

    def score(chip, wide, start, size, part):
        cc = pl.ds(pl.multiple_of(start, size), size)
        s = lax.dot_general(
            c_all[cc], q_all[pl.ds(pl.multiple_of(chip * pair, wide), wide)],
            (((1,), (1,)), ((), ())), preferred_element_type=F32,
        ) * (scaling * LOG2E)
        for x in range(0, wide, LANES):
            qq = pl.ds(pl.multiple_of(chip * pair + x, LANES), LANES)
            tile = s[:, x : x + LANES]
            s_all[cc, qq] = tile

            def put(i, row):
                tables[chip + x // pair, part, i : i + 1, x % pair : x % pair + LANES] = row

            statistics(tile, g_all[cc, qq], put)

    def near(k, dm):
        score(at.chip(at.visit(k), dm), pair, at.p * half, half, 0)

    def far(k, r):
        score(2 * at.visit(k), quad, c_first(r), parts[r][2], r + 1)

    def each(last, task):
        lax.fori_loop(0, last, lambda j, c: (task(j), c)[1], 0)

    def stat_copy(block):
        return remote(stats.at[block], got.at[at.me], s_send.at[block], s_recv.at[at.me], at.dev(block))

    def join(ks):
        todo = [2 * at.visit(k) + m for k in ks for m in range(2)]
        for chip in todo:
            tabs = [tables[chip, h] for h in range(n_far + 1)]
            top = tabs[0][:8]
            for tab in tabs[1:]:
                top = jnp.maximum(top, tab[:8])
            mass = sum(tab[8:] * jnp.exp2(tab[:8] - top) for tab in tabs)
            count = counts[:, span(chip, pair)]
            for c in range(2):
                here = slice(c * rows, (c + 1) * rows)
                stats[chip * 2 + c, :8] = (top + count[:8])[:, here]
                stats[chip * 2 + c, 8:] = (mass + count[8:])[:, here]
        for chip in todo:
            for c in range(2):
                @pl.when(chip * 2 + c != at.me)
                def _():
                    stat_copy(chip * 2 + c).start()

    partner(0, 0)
    near(0, 0)
    if outs > 1:
        forward(1, 0, True, [0])

    def step(u, carry):
        forward(u, 0, True, range(1, SUBS))
        forward(u - 1, 1, True)
        partner(u - 1, 1)
        near(u - 1, 1)

        @pl.when(u + 1 < outs)
        def _():
            forward(u + 1, 0, True, [0])

        partner(u, 0)
        near(u, 0)

        @pl.when(u == 2)
        def _():
            for r in range(early):
                c_arrived(r)

        @pl.when(u >= 2)
        def _():
            for r in range(early):
                far(u - 2, r)

        return carry

    lax.fori_loop(1, outs, step, 0)
    if outs < 3:
        for r in range(early):
            c_arrived(r)
    for k in range(max(outs - 2, 0), outs - 1):
        for r in range(early):
            far(k, r)
    for r in range(early, n_far):
        if r == n_far - early:
            forward(outs - 1, 1, True)
        c_arrived(r)
        each(outs - 1, lambda k, r=r: far(k, r))
    if n_far == early:
        forward(outs - 1, 1, True)
    join(range(outs - 1))
    partner(outs - 1, 1)
    near(outs - 1, 1)
    for r in range(n_far):
        far(outs - 1, r)
    join([outs - 1])

    others = [lax.rem(at.me + d, n_col) for d in range(1, n_col)]
    got[at.me] = stats[at.me]
    for o in others:
        remote(stats.at[o], got.at[o], s_send.at[o], s_recv.at[o], at.dev(at.me)).wait_recv()
    mine[...] = finish(got, n_col, cols, columns)

    def merged_copy(o):
        return remote(mine, merged.at[at.me], m_send.at[o], m_recv.at[at.me], at.dev(o))

    for o in others:
        merged_copy(o).start()
    merged[at.me] = mine[...]
    for o in others:
        remote(mine, merged.at[o], m_send.at[o], m_recv.at[o], at.dev(at.me)).wait_recv()

    def slope(chip, start, size):
        qq = span(chip, pair)
        table = jnp.concatenate([merged[2 * chip], merged[2 * chip + 1]], axis=1)
        few = pair // LANES
        w = [w_ref[pl.ds(chip * few + x, 1), :] for x in range(few)]
        w = jnp.concatenate(w, axis=1)
        for x in range(0, pair, LANES):
            loss_ref[pl.ds(chip * (pair // LANES) + x // LANES, 1), :] = table[G : G + 1, x : x + LANES]

        def body(j, carry):
            cc = pl.ds(pl.multiple_of(start + j * chunk, chunk), chunk)
            g = g_all[cc, qq]
            off = pick(table, g)
            slopes[cc, qq] = (w * jnp.exp2(s_all[cc, qq] + off) - w).astype(BF16)
            return carry

        if size == chunk:
            body(0, 0)
        else:
            lax.fori_loop(0, size // chunk, body, 0)

    def k_copy(chip):
        return remote(
            q_part.at[chip, lax.rem(at.core + 1, 2)], core_got.at[chip], k_send.at[chip], k_recv.at[chip],
            at.dev(at.block(at.out, 0, 1)),
        )

    def q_grad(t):
        out, dm = at.item(t)
        chip = at.chip(out, dm)
        part = lax.dot_general(
            slopes[:, span(chip, pair)], c_all[...], (((0,), (0,)), ((), ())), preferred_element_type=F32
        ) * scaling
        q_part[chip] = part.astype(BF16).reshape(2, rows, width)
        k_copy(chip).start()

    def sub_rows(s):
        return pl.ds(s * sub, sub)

    def y_copy(out, s):
        return remote(
            q_part.at[at.chip(out, 1), at.core, sub_rows(s)], y_got.at[out, sub_rows(s)],
            y_send.at[out, s], y_recv.at[out, s], at.dev(at.block(at.out, 1, 0)),
        )

    def cross(out):
        chip = at.chip(out, 1)
        k_copy(chip).wait_recv()
        for s in range(SUBS):
            rr = sub_rows(s)
            both = q_part[chip, at.core, rr].astype(F32) + core_got[chip, rr].astype(F32)
            q_part[chip, at.core, rr] = both.astype(BF16)
            y_copy(out, s).start()

    def z_copy(out, s):
        toward = jnp.where(out > at.out, at.out + 1, at.out - 1)
        slot = jnp.where((out < at.out) & (toward == out), outs, out)
        return remote(
            z_part.at[out, sub_rows(s)], z_got.at[slot, sub_rows(s)],
            z_send.at[out, s], z_recv.at[slot, s], at.dev(at.block(toward, 0, 0)),
        )

    def z_add(slot, s):
        ref = z_got.at[slot, sub_rows(s)]
        remote(ref, ref, z_send.at[0, s], z_recv.at[slot, s], at.dev(at.me)).wait_recv()
        acc[...] += z_got[slot, sub_rows(s)].astype(F32)

    def gather_row(out, s):
        chip = at.chip(out, 0)
        rr = sub_rows(s)
        ref = y_got.at[out, rr]
        remote(ref, ref, y_send.at[out, s], y_recv.at[out, s], at.dev(at.me)).wait_recv()
        acc[...] = (
            q_part[chip, at.core, rr].astype(F32)
            + core_got[chip, rr].astype(F32)
            + y_got[out, rr].astype(F32)
        )

    def chain(v):
        out = at.visit(v)
        k_copy(at.chip(out, 0)).wait_recv()
        behind = ((out > at.out) & (at.out > 0)) | ((out < at.out) & (at.out < outs - 1))
        for s in range(SUBS):
            gather_row(out, s)

            @pl.when(behind)
            def _():
                z_add(out, s)

            z_part[out, sub_rows(s)] = acc[...].astype(BF16)
            z_copy(out, s).start()

    per = half // chunk
    n_x = per * (n_pb - 1)

    def x_copy(r):
        d, j = 1 + r // per, lax.rem(r, per)
        other = lax.rem(at.p + d, n_pb)
        rr = pl.ds(pl.multiple_of(j * chunk, chunk), chunk)
        return remote(
            c_part.at[r], c_got.at[d - 1, rr], x_send.at[r], x_recv.at[r], {"pb": other, "col": at.me}
        )

    def c_grad(start):
        here = slopes[pl.ds(pl.multiple_of(start, chunk), chunk), :]
        return jnp.dot(here, q_all[...], preferred_element_type=F32) * scaling

    def c_far(r):
        other = lax.rem(at.p + 1 + r // per, n_pb)
        c_part[r] = c_grad(other * half + lax.rem(r, per) * chunk).astype(BF16)
        x_copy(r).start()

    def slope_first(i, carry):
        slope(i, lax.rem(at.p + 1, n_pb) * half, chunk)
        return carry

    def slope_step(i, carry):
        out, dm = at.item(i)
        slope(at.chip(out, dm), 0, cols)

        @pl.when(i == 0)
        def _():
            q_grad(0)

        @pl.when(i == 2)
        def _():
            cross(at.visit(outs - 1))

        return carry

    lax.fori_loop(0, chips, slope_first, 0)
    c_far(0)
    lax.fori_loop(0, chips, slope_step, 0)

    edge = (at.out == 0) | (at.out == outs - 1)

    def grad_step(j, carry):
        @pl.when((j > 0) & (j < n_x))
        def _():
            c_far(j)

        @pl.when(j + 1 < chips)
        def _():
            q_grad(j + 1)

        @pl.when((j >= 1) & (lax.rem(j, 2) == 1) & (j < chips - 1))
        def _():
            cross(at.item(j)[0])

        @pl.when((j == 2) & edge)
        def _():
            chain(outs - 1)

        return carry

    lax.fori_loop(0, max(n_x, chips - 1), grad_step, 0)

    def c_near(j, carry):
        c_own[pl.ds(pl.multiple_of(j * chunk, chunk), chunk)] = c_grad(at.p * half + j * chunk)
        return carry

    def chain_step(i, carry):
        @pl.when((i > 0) | jnp.logical_not(edge))
        def _():
            chain(outs - 1 - i)

        @pl.when((i == 0) & jnp.logical_not(edge) | (i == min(1, outs - 2)) & edge)
        def _():
            lax.fori_loop(0, per, c_near, 0)

        return carry

    lax.fori_loop(0, outs - 1, chain_step, 0)
    k_copy(at.chip(at.out, 0)).wait_recv()
    for s in range(SUBS):
        gather_row(at.out, s)

        @pl.when(at.out > 0)
        def _():
            z_add(at.out, s)

        @pl.when(at.out < outs - 1)
        def _():
            z_add(outs, s)

        q_out[sub_rows(s), :] = acc[...].astype(BF16)

    loss_copy = pltpu.make_async_copy(loss_ref, loss_hbm, out_sem.at[0])
    q_end_copy = pltpu.make_async_copy(q_out, q_end, out_sem.at[1])
    loss_copy.start()
    q_end_copy.start()

    def c_end_copy(j):
        rr = pl.ds(pl.multiple_of(j * chunk, chunk), chunk)
        return pltpu.make_async_copy(c_out.at[rr], c_end.at[rr], out_sem.at[2 + j])

    def c_finish(j, carry):
        rr = pl.ds(pl.multiple_of(j * chunk, chunk), chunk)
        total = c_own[rr]
        for d in range(1, n_pb):
            r = (d - 1) * per + j
            ref = c_got.at[d - 1, rr]
            remote(ref, ref, x_send.at[r], x_recv.at[r], at.dev(at.me)).wait_recv()
            total = total + c_got[d - 1, rr].astype(F32)
        c_out[rr] = total.astype(BF16)
        c_end_copy(j).start()
        return carry

    lax.fori_loop(0, per, c_finish, 0)

    def drain(k, carry):
        for dm in range(2):
            forward(k, dm, False)
        out = at.visit(k)
        for dm in range(2):
            k_copy(at.chip(out, dm)).wait_send()
        for s in range(SUBS):
            y_copy(out, s).wait_send()

            @pl.when(k > 0)
            def _():
                z_copy(out, s).wait_send()

        return carry

    lax.fori_loop(0, outs, drain, 0)
    for r in range(n_far):
        c_copy(r).wait_send()
    for o in others:
        stat_copy(o).wait_send()
        merged_copy(o).wait_send()
    lax.fori_loop(0, n_x, lambda r, c: (x_copy(r).wait_send(), c)[1], 0)
    loss_copy.wait()
    q_end_copy.wait()
    lax.fori_loop(0, per, lambda j, c: (c_end_copy(j).wait(), c)[1], 0)


def copy_kernel(*refs):
    n = (len(refs) - 2) // 3
    sources, outs, held = refs[:n], refs[n : 2 * n], refs[2 * n : 3 * n]
    into, back = refs[3 * n :]
    reads = [pltpu.make_async_copy(a, h, into.at[i]) for i, (a, h) in enumerate(zip(sources, held))]
    writes = [pltpu.make_async_copy(h, o, back.at[i]) for i, (h, o) in enumerate(zip(held, outs))]
    for read in reads:
        read.start()
    for read, write in zip(reads, writes):
        read.wait()
        write.start()
    for write in writes:
        write.wait()


def settle(arrays):
    hbm = pl.BlockSpec(memory_space=pl.ANY)
    dma = pltpu.SemaphoreType.DMA((len(arrays),))
    return pl.pallas_call(
        copy_kernel,
        out_shape=tuple(jax.ShapeDtypeStruct(a.shape, a.dtype) for a in arrays),
        in_specs=[hbm] * len(arrays),
        out_specs=(hbm,) * len(arrays),
        scratch_shapes=[pltpu.VMEM(a.shape, a.dtype) for a in arrays] + [dma, dma],
        name="settle",
    )(*arrays)


def local(queries, candidates, grades, query_weights):
    n_col, n_pb = lax.axis_size("col"), lax.axis_size("pb")
    rows, width = queries.shape
    half = candidates.shape[0]
    tall, cols = grades.shape
    scaling = 1.0 / math.sqrt(width)
    n_far = len(far_parts_of(half, n_pb))
    outs, chips = n_col // 4, n_col // 2
    chunk = min(LANES, half)
    n_x = half // chunk * (n_pb - 1)
    sub = rows // SUBS
    dma = pltpu.SemaphoreType.DMA
    vmem = pl.BlockSpec(memory_space=pltpu.VMEM)
    hbm = pl.BlockSpec(memory_space=pl.ANY)
    outputs = pl.pallas_call(
        functools.partial(kernel, n_col, n_pb, scaling, cols * n_col),
        out_shape=(
            jax.ShapeDtypeStruct((tall // LANES, LANES), F32),
            jax.ShapeDtypeStruct((rows, width), BF16),
            jax.ShapeDtypeStruct((half, width), BF16),
        ),
        in_specs=[hbm, hbm, hbm, vmem],
        out_specs=(hbm, hbm, hbm),
        scratch_shapes=[
            pltpu.VMEM((tall // LANES, LANES), F32),
            pltpu.VMEM((rows, width), BF16),
            pltpu.VMEM((half, width), BF16),
            pltpu.VMEM((tall, width), BF16),
            pltpu.VMEM((cols, width), BF16),
            pltpu.VMEM((tall, cols), jnp.int32),
            pltpu.VMEM((cols, tall), jnp.int32),
            pltpu.VMEM((cols, tall), F32),
            pltpu.VMEM((cols, tall), BF16),
            pltpu.VMEM((chips, 1 + n_far, STATS, 2 * rows), F32),
            pltpu.VMEM((STATS, tall), F32),
            pltpu.VMEM((n_col, STATS, rows), F32),
            pltpu.VMEM((n_col, STATS, rows), F32),
            pltpu.VMEM((8, rows), F32),
            pltpu.VMEM((n_col, 8, rows), F32),
            pltpu.VMEM((chips, 2, rows, width), BF16),
            pltpu.VMEM((chips, rows, width), BF16),
            pltpu.VMEM((outs, rows, width), BF16),
            pltpu.VMEM((outs + 1, rows, width), BF16),
            pltpu.VMEM((outs, rows, width), BF16),
            pltpu.VMEM((sub, width), F32),
            pltpu.VMEM((n_x, chunk, width), BF16),
            pltpu.VMEM((half, width), F32),
            pltpu.VMEM((n_pb - 1, half, width), BF16),
            dma((2 + half // chunk,)),
            dma((2,)),
            dma((tall // (8 * LANES),)),
            dma((n_col, 4, SUBS)),
            dma((n_col, SUBS)),
            dma((n_far,)),
            dma((n_far,)),
            dma((n_col,)),
            dma((n_col,)),
            dma((n_col,)),
            dma((n_col,)),
            dma((chips,)),
            dma((chips,)),
            dma((outs, SUBS)),
            dma((outs, SUBS)),
            dma((outs, SUBS)),
            dma((outs + 1, SUBS)),
            dma((n_x,)),
            dma((n_x,)),
        ],
        compiler_params=pltpu.CompilerParams(
            collective_id=0, has_side_effects=True, vmem_limit_bytes=62 * 2**20
        ),
        name="listmle",
    )(queries, candidates, grades, query_weights.reshape(tall // LANES, LANES))
    losses, cand_grad, query_grad = settle((outputs[0], outputs[2], outputs[1]))
    return (losses.reshape(-1), query_grad, cand_grad)


def solution(mesh):
    in_specs = (P(("pb", "col"), None), P(("col", "pb"), None), P("pb", "col"), P("pb"))
    out_specs = (P("pb"), P(("pb", "col"), None), P(("col", "pb"), None))
    return jax.shard_map(local, mesh=mesh, in_specs=in_specs, out_specs=out_specs, check_vma=False)
```
